32 devices in a mesh: spatial: 8 (over y, x, core), fsdp: 4 (over z).
Axes of the slice: x: 2, y: 2, z: 4, core: 2. Of those that a mesh axis runs over, the one named last changes fastest.
Arguments:
- features: bfloat16 [4, 32, 64, 640], P('fsdp', 'spatial'), may hold values from -60 to 60
- step_index: int32 [1], replicated, may hold values from 0 to 49
- roster: float32 [50], replicated, may hold values from 1 to 999
- time_weight: float32 [320, 1280], replicated, may hold values from -0.3125 to 0.3125
- temb_weight: float32 [1280, 640], replicated, may hold values from -0.15625 to 0.15625
- norm_gains: float32 [3, 640], replicated, may hold values from 0.1 to 1.9
- conv_first: bfloat16 [5760, 640], P(None, 'fsdp'), may hold values from -0.078125 to 0.078125
- conv_second: bfloat16 [5760, 640], P(None, 'fsdp'), may hold values from -0.078125 to 0.078125
- attn_weight: bfloat16 [640, 1920], P(None, 'fsdp'), may hold values from -0.15811388 to 0.15811388
- out_weight: bfloat16 [640, 640], P(None, 'fsdp'), may hold values from -0.25 to 0.25
Outputs:
- refined: bfloat16 [4, 32, 64, 640], P('fsdp', 'spatial')
The draws below stay inside these ranges and needn't reach their ends.
All inputs are finite; a program needn't handle non-finite values.
Results may differ from the reference program's by a relative error of at most 0.02.
Values may be sent and summed in bfloat16 or wider, within the bound.
No kernel may reach another device: no remote copies, remote signals or barrier semaphores. Data moves between devices by JAX's collectives and lax.ppermute only.
A program may use at most 192 MiB of HBM per device.

```python
import math
import jax
import jax.numpy as jnp
from jax import lax

C = 640
TEMB = 1280
FREQ = 320
HEAD_DIM = 64
GROUPS = 32
STEPS = 50
COLS = 64
ROWS = 32
SAMPLES = 4


def draw_features(key, part):
    keys_list = jax.random.split(key, 3)
    positions = jnp.arange(ROWS, dtype=jnp.float32)
    trend = 3.0 ** (positions / max(ROWS - 1, 1))
    rough = jnp.exp(jax.random.uniform(keys_list[0], (SAMPLES, ROWS), jnp.float32, 0.0, math.log(3.3)))
    channel_scale = jnp.exp(jax.random.uniform(keys_list[1], (C,), jnp.float32, 0.0, math.log(10.0)))
    scaling = (trend[None, :] * rough)[:, :, None, None] * channel_scale[None, None, None, :] / 3.0
    values = jax.random.normal(keys_list[2], (SAMPLES, ROWS, COLS, C), jnp.float32) * scaling
    return jnp.clip(values, -60.0, 60.0).astype(jnp.bfloat16)


def draw_attn_weight(key, part):
    matrix = jax.random.truncated_normal(key, -3.9, 3.9, (C, 3 * C), jnp.float32) / math.sqrt(C)
    return matrix.astype(jnp.bfloat16)


def block_scale(own_key, shape, cuts, low, high):
    gain, own = 1.0, jax.random.fold_in(own_key, 6)
    for position, shards_of in cuts:
        draws = jnp.exp(jax.random.uniform(jax.random.fold_in(own, position), (shards_of,), jnp.float32, low / len(cuts), high / len(cuts)))
        gain = gain * jnp.repeat(draws, shape[position] // shards_of).reshape([-1 if axis == position else 1 for axis in range(len(shape))])
    return gain


def gaussian(rng, dims, width, limit, cuts=(), kind=jnp.bfloat16):
    values = jax.random.normal(rng, dims, jnp.float32) * width
    if len(cuts) > 0:
        values = block_scale(rng, dims, cuts, -0.22, 0.18) * values
    return jnp.clip(values, min=-limit, max=limit).astype(kind)


def setup_inputs(seed: int = 0) -> dict:
    streams_of = jax.random.split(jax.random.key(seed), 11)
    features = draw_features(jax.random.fold_in(streams_of[10], 71), 0)
    step_index = jax.random.randint(streams_of[1], (1,), 0, STEPS).astype(jnp.int32)
    roster = jnp.clip(jax.random.uniform(streams_of[2], (STEPS,), jnp.float32, 1.0, 999.0), 1.0, 999.0)
    time_weight = gaussian(streams_of[3], (FREQ, TEMB), FREQ ** -0.5, 0.3125, (), jnp.float32)
    temb_weight = gaussian(streams_of[4], (TEMB, C), TEMB ** -0.5, 0.15625, (), jnp.float32)
    norm_gains = jnp.clip(1.0 + 0.18 * jax.random.normal(streams_of[5], (3, C), jnp.float32), 0.1, 1.9)
    conv_first = gaussian(streams_of[6], (9 * C, C), (9 * C) ** -0.5, 0.078125, ((1, 4),))
    conv_second = gaussian(streams_of[7], (9 * C, C), (9 * C) ** -0.5, 0.078125, ((1, 4),))
    attn_weight = draw_attn_weight(jax.random.fold_in(streams_of[10], 71), 0)
    out_weight = gaussian(streams_of[9], (C, C), C ** -0.5, 0.25, ((1, 4),))
    return dict(features=features, step_index=step_index, roster=roster, time_weight=time_weight, temb_weight=temb_weight, norm_gains=norm_gains, conv_first=conv_first, conv_second=conv_second, attn_weight=attn_weight, out_weight=out_weight)


EPSILON = 1e-05

def time_bias(step_index, roster, time_weight, temb_weight):
    picked = jnp.arange(roster.shape[0], dtype=jnp.int32) == step_index[0]
    moment = jnp.sum(jnp.where(picked, roster, jnp.zeros_like(roster)))
    half_len = time_weight.shape[0] // 2
    frequency = jnp.exp(-math.log(10000.0) * jnp.arange(half_len, dtype=jnp.float32) / half_len)
    angles = moment * frequency
    embedding = jnp.concatenate([jnp.cos(angles), jnp.sin(angles)])[None, :]
    time_hidden = jax.nn.silu(jnp.dot(embedding, time_weight, precision=lax.Precision.HIGHEST))
    return jnp.dot(time_hidden, temb_weight, precision=lax.Precision.HIGHEST)[0]

def channel_groups(per_channel):
    return lax.optimization_barrier(jnp.sum(per_channel.reshape(per_channel.shape[0], GROUPS, -1), axis=2))

def spread_groups(per_group, channels):
    return jnp.repeat(per_group, channels // GROUPS, axis=1)

def group_norm(values, gain_row):
    samples, height, columns, channels = values.shape
    entries = height * columns * (channels // GROUPS)
    group_mean = channel_groups(lax.optimization_barrier(jnp.sum(values, axis=(1, 2)))) / entries
    centered = values - spread_groups(group_mean, channels)[:, None, None, :]
    spread = channel_groups(lax.optimization_barrier(jnp.sum(centered * centered, axis=(1, 2)))) / entries
    scales = spread_groups(lax.rsqrt(spread + EPSILON), channels)
    return centered * scales[:, None, None, :] * gain_row

def convolve(padded, weight):
    samples, rows_pad, cols_pad, channels = padded.shape
    height, columns = (rows_pad - 2, cols_pad - 2)
    summed = jnp.zeros((samples * height * columns, weight.shape[1]), jnp.float32)
    for offset in range(9):
        row_shift, col_shift = (offset // 3, offset % 3)
        window = padded[:, row_shift:row_shift + height, col_shift:col_shift + columns, :]
        window = window.reshape(samples * height * columns, channels)
        tap_rows = weight[offset * channels:(offset + 1) * channels]
        summed = summed + jnp.dot(window, tap_rows, preferred_element_type=jnp.float32)
    return summed.reshape(samples, height, columns, weight.shape[1])

def attend_one(projected):
    length, triple = projected.shape
    channels = triple // 3
    heads = channels // HEAD_DIM
    stacked = projected.reshape(length, 3, heads, HEAD_DIM).transpose(2, 1, 0, 3)

    def one_head(triplet):
        scores = jnp.dot(triplet[0], triplet[1].T, preferred_element_type=jnp.float32) * HEAD_DIM ** (-0.5)
        shifted = jnp.exp(scores - lax.optimization_barrier(jnp.max(scores, axis=1, keepdims=True)))
        totals = lax.optimization_barrier(jnp.sum(shifted, axis=1, keepdims=True))
        return jnp.dot(shifted.astype(jnp.bfloat16), triplet[2], preferred_element_type=jnp.float32) / totals
    heads_out = lax.map(one_head, stacked)
    return heads_out.transpose(1, 0, 2).reshape(length, channels).astype(jnp.bfloat16)

def reference(features, step_index, roster, time_weight, temb_weight, norm_gains, conv_first, conv_second, attn_weight, out_weight):
    bias_row = time_bias(step_index, roster, time_weight, temb_weight)
    start = features.astype(jnp.float32)
    pad_spec = ((0, 0), (1, 1), (1, 1), (0, 0))
    first_input = jax.nn.silu(group_norm(start, norm_gains[0])).astype(jnp.bfloat16)
    first_out = convolve(jnp.pad(first_input, pad_spec), conv_first) + bias_row
    second_input = jax.nn.silu(group_norm(first_out, norm_gains[1])).astype(jnp.bfloat16)
    block_out = (start + convolve(jnp.pad(second_input, pad_spec), conv_second)).astype(jnp.bfloat16)
    normed = group_norm(block_out.astype(jnp.float32), norm_gains[2]).astype(jnp.bfloat16)
    samples, height, columns, channels = normed.shape
    flat_tokens = normed.reshape(samples * height * columns, channels)
    projected = jnp.dot(flat_tokens, attn_weight, preferred_element_type=jnp.float32).astype(jnp.bfloat16)
    projected = projected.reshape(samples, height * columns, 3 * channels)
    mixed = lax.map(attend_one, projected)
    attention = jnp.dot(mixed.reshape(samples * height * columns, channels), out_weight, preferred_element_type=jnp.float32)
    refined = block_out.astype(jnp.float32) + attention.reshape(samples, height, columns, channels)
    return refined.astype(jnp.bfloat16)
```

```python
import math

import jax
import jax.numpy as jnp
from jax import lax
from jax.experimental import pallas as pl
from jax.experimental.pallas import tpu as pltpu
from jax.sharding import PartitionSpec as P

HEAD_DIM = 64
GROUPS = 32
EPSILON = 1e-05
LANES = 128
HIGHEST = lax.Precision.HIGHEST


NT = (((1,), (1,)), ((), ()))
TN = (((0,), (0,)), ((), ()))


def call(body, out_shape, scratch=(), scalars=0, flops=0):
    def run(*operands):
        specs = [
            pl.BlockSpec(memory_space=pltpu.SMEM if i < scalars else pltpu.VMEM)
            for i in range(len(operands))
        ]
        outs = jax.tree.map(lambda _: pl.BlockSpec(memory_space=pltpu.VMEM), out_shape)
        return pl.pallas_call(
            body,
            out_shape=out_shape,
            in_specs=specs,
            out_specs=outs,
            scratch_shapes=list(scratch),
            compiler_params=pltpu.CompilerParams(vmem_limit_bytes=60 * 2**20),
            cost_estimate=pl.CostEstimate(flops=flops, transcendentals=0, bytes_accessed=0)
            if flops
            else None,
        )(*operands)

    return run


def shift(values, axis, step):
    count = lax.axis_size(axis)
    return lax.ppermute(values, axis, [(i, (i + step) % count) for i in range(count)])


def silu(v):
    return v / (1.0 + jnp.exp(-v))


def time_bias(step_index, roster, time_weight, temb_columns):
    picked = jnp.arange(roster.shape[0], dtype=jnp.int32) == step_index[0]
    moment = jnp.sum(jnp.where(picked, roster, jnp.zeros_like(roster)))
    half_len = time_weight.shape[0] // 2
    frequency = jnp.exp(-math.log(10000.0) * jnp.arange(half_len, dtype=jnp.float32) / half_len)
    angles = moment * frequency
    embedding = jnp.concatenate([jnp.cos(angles), jnp.sin(angles)])[None, :]
    time_hidden = jax.nn.silu(jnp.dot(embedding, time_weight, precision=HIGHEST))
    return jnp.dot(time_hidden, temb_columns, precision=HIGHEST)[0]


def same_group(rows, block, kept, width):
    index = jnp.arange(rows)
    real = index % block < kept
    group = (index // block * kept + index % block) // width
    return ((group[:, None] == group[None, :]) & real[:, None] & real[None, :]).astype(jnp.float32)


def local_stats(features, groups, width):
    samples, length, channels = features.shape

    def body(x_ref, g_ref, o_ref):
        for i in range(samples):
            v = x_ref[i].astype(jnp.float32)
            total = jnp.broadcast_to(jnp.sum(v, axis=0, keepdims=True), (8, channels))
            mean = jnp.dot(total, g_ref[...], precision=HIGHEST)[:1] / (length * width)
            c = v - mean
            squares = jnp.broadcast_to(jnp.sum(c * c, axis=0, keepdims=True), (8, channels))
            o_ref[i : i + 1] = mean
            o_ref[samples + i : samples + i + 1] = jnp.dot(
                squares, g_ref[...], precision=HIGHEST
            )[:1]

    return call(body, jax.ShapeDtypeStruct((2 * samples, channels), jnp.float32))(features, groups)


def merge_stats(parts, gain, entries):
    devices, rows, channels = parts.shape
    count = rows // 2

    def body(p_ref, g_ref, o_ref):
        mean = p_ref[0, :count]
        for d in range(1, devices):
            mean = mean + p_ref[d, :count]
        mean = mean / devices
        squares = jnp.zeros_like(mean)
        for d in range(devices):
            away = p_ref[d, :count] - mean
            squares = squares + p_ref[d, count:] + entries * (away * away)
        o_ref[:count] = mean
        o_ref[count:] = lax.rsqrt(squares / (entries * devices) + EPSILON) * g_ref[...]

    return call(body, jax.ShapeDtypeStruct((rows, channels), jnp.float32))(parts, gain)


def column_shift(y, shard, width):
    lane = lax.broadcasted_iota(jnp.int32, (shard, LANES), 1) % width
    tiles = []
    for start in range(0, y.shape[1], LANES):
        left = y[:shard, start : start + LANES]
        right = y[2 * shard :, start : start + LANES]
        tiles.append(
            y[shard : 2 * shard, start : start + LANES]
            + jnp.where(lane > 0, pltpu.roll(left, 1, axis=1), 0.0)
            + jnp.where(lane < width - 1, pltpu.roll(right, LANES - 1, axis=1), 0.0)
        )
    return jnp.concatenate(tiles, axis=1)


def first_conv(ends, edges, mids, above, below, stats, weight, bias, groups, pick, eye, width, group):
    n = len(edges)
    samples, edge, channels = edges[0].shape
    mid = mids[0].shape[1]
    shard = bias.shape[0]
    count = n * samples
    inner = mid // width
    length = edge + mid

    def body(*refs):
        ends_ref = refs[0]
        e_refs, m_refs, s_refs = refs[1 : 1 + n], refs[1 + n : 1 + 2 * n], refs[1 + 2 * n : 1 + 3 * n]
        a_ref, b_ref, w_ref, t_ref, g_ref, p_ref, i_ref = refs[1 + 3 * n : 8 + 3 * n]
        eo_ref, mo_ref, so_ref, fe_ref, fm_ref, buf = refs[8 + 3 * n :]
        has_above = ends_ref[0].astype(jnp.float32)
        has_below = ends_ref[1].astype(jnp.float32)
        lane = lax.broadcasted_iota(jnp.int32, (shard, LANES), 1)
        columns = jnp.zeros((shard, LANES), jnp.float32)
        for j in range(n):
            for i in range(samples):
                q = j * samples + i
                mean = s_refs[j][i : i + 1]
                scale = s_refs[j][samples + i : samples + i + 1]

                def act(x):
                    return silu((x.astype(jnp.float32) - mean) * scale)

                e = e_refs[j][i]
                m = m_refs[j][i]
                ea = act(e).astype(jnp.bfloat16)
                buf[:width] = (act(a_ref[q]) * has_above).astype(jnp.bfloat16)
                buf[width : 2 * width] = ea[:width]
                buf[2 * width : 2 * width + mid] = act(m).astype(jnp.bfloat16)
                buf[2 * width + mid : 3 * width + mid] = ea[width:]
                buf[3 * width + mid :] = (act(b_ref[q]) * has_below).astype(jnp.bfloat16)
                y = jnp.zeros((3 * shard, length), jnp.float32)
                for a in range(3):
                    window = jnp.concatenate(
                        [
                            buf[a * width : (a + 1) * width],
                            buf[(a + 1 + inner) * width : (a + 2 + inner) * width],
                            buf[(a + 1) * width : (a + 1 + inner) * width],
                        ],
                        axis=0,
                    )
                    y = y + lax.dot_general(w_ref[a], window, NT, preferred_element_type=jnp.float32)
                out = column_shift(y, shard, width) + t_ref[:, :1]
                eo_ref[:, q * edge : (q + 1) * edge] = out[:, :edge].astype(jnp.bfloat16)
                mo_ref[:, q * mid : (q + 1) * mid] = out[:, edge:].astype(jnp.bfloat16)
                fe_ref[:, q * edge : (q + 1) * edge] = lax.dot_general(
                    p_ref[...], e, NT, preferred_element_type=jnp.float32
                ).astype(jnp.bfloat16)
                fm_ref[:, q * mid : (q + 1) * mid] = lax.dot_general(
                    p_ref[...], m, NT, preferred_element_type=jnp.float32
                ).astype(jnp.bfloat16)
                total = jnp.broadcast_to(jnp.sum(out, axis=1, keepdims=True), (shard, LANES))
                center = jnp.dot(g_ref[...], total, precision=HIGHEST) / (length * group)
                c = out - center[:, :1]
                squares = jnp.broadcast_to(jnp.sum(c * c, axis=1, keepdims=True), (shard, LANES))
                columns = jnp.where(lane == q, center, columns)
                columns = jnp.where(
                    lane == count + q, jnp.dot(g_ref[...], squares, precision=HIGHEST), columns
                )
        so_ref[...] = lax.dot_general(i_ref[...], columns, NT, precision=HIGHEST)

    out_shape = (
        jax.ShapeDtypeStruct((shard, count * edge), jnp.bfloat16),
        jax.ShapeDtypeStruct((shard, count * mid), jnp.bfloat16),
        jax.ShapeDtypeStruct((2 * count, shard), jnp.float32),
        jax.ShapeDtypeStruct((shard, count * edge), jnp.bfloat16),
        jax.ShapeDtypeStruct((shard, count * mid), jnp.bfloat16),
    )
    scratch = [pltpu.VMEM((length + 2 * width, channels), jnp.bfloat16)]
    return call(body, out_shape, scratch, scalars=1, flops=6 * count * length * channels * 3 * shard)(
        ends, *edges, *mids, *stats, above, below, weight, bias, groups, pick, eye
    )


def second_conv(ends, edges, mids, stats, above, below, weight, own_edges, own_mids, eye, samples, width):
    n = len(edges)
    shard = edges[0].shape[0]
    count = n * samples
    edge, mid = edges[0].shape[1] // count, mids[0].shape[1] // count
    length = edge + mid

    def body(*refs):
        ends_ref = refs[0]
        e_refs, m_refs, s_refs = refs[1 : 1 + n], refs[1 + n : 1 + 2 * n], refs[1 + 2 * n : 1 + 3 * n]
        a_ref, b_ref, w_ref, fe_ref, fm_ref, i_ref = refs[1 + 3 * n : 7 + 3 * n]
        o_ref, buf = refs[7 + 3 * n :]
        has_above = ends_ref[0].astype(jnp.float32)
        has_below = ends_ref[1].astype(jnp.float32)
        low = lax.broadcasted_iota(jnp.int32, (shard, edge), 1) < width
        columns = [
            lax.dot_general(i_ref[...], s_refs[j][...], NT, precision=HIGHEST) for j in range(n)
        ]
        for t in range(n):
            for i in range(samples):
                for j in range(n):
                    q = (t - j) % n * samples + i
                    mean = columns[j][:, q : q + 1]
                    scale = columns[j][:, count + q : count + q + 1]

                    def act(x):
                        return silu((x.astype(jnp.float32) - mean) * scale)

                    rows = slice(j * shard, (j + 1) * shard)
                    cut = slice(q * edge, (q + 1) * edge)
                    e = act(e_refs[j][:, cut])
                    m = act(m_refs[j][:, q * mid : (q + 1) * mid])
                    top = pltpu.roll(act(a_ref[rows, cut]), width, axis=1) * has_above
                    bottom = pltpu.roll(act(b_ref[rows, cut]), width, axis=1) * has_below
                    turned = pltpu.roll(m, width, axis=1)
                    buf[0, rows, :edge] = jnp.where(low, top, m).astype(jnp.bfloat16)
                    buf[0, rows, edge:] = jnp.where(low, e, turned).astype(jnp.bfloat16)
                    buf[1, rows, :edge] = e.astype(jnp.bfloat16)
                    buf[1, rows, edge:] = m.astype(jnp.bfloat16)
                    buf[2, rows, :edge] = jnp.where(low, m, bottom).astype(jnp.bfloat16)
                    buf[2, rows, edge:] = jnp.where(low, turned, e).astype(jnp.bfloat16)
                y = jnp.zeros((3 * shard, length), jnp.float32)
                for a in range(3):
                    y = y + jnp.dot(w_ref[a], buf[a], preferred_element_type=jnp.float32)
                out = column_shift(y, shard, width)
                q = t * samples + i
                o_ref[t, i, :, :edge] = (
                    out[:, :edge] + fe_ref[:, q * edge : (q + 1) * edge].astype(jnp.float32)
                ).astype(jnp.bfloat16)
                o_ref[t, i, :, edge:] = (
                    out[:, edge:] + fm_ref[:, q * mid : (q + 1) * mid].astype(jnp.float32)
                ).astype(jnp.bfloat16)

    return call(
        body,
        jax.ShapeDtypeStruct((n, samples, shard, length), jnp.bfloat16),
        [pltpu.VMEM((3, n * shard, length), jnp.bfloat16)],
        scalars=1,
        flops=6 * count * length * n * shard * 3 * shard,
    )(ends, *edges, *mids, *stats, above, below, weight, own_edges, own_mids, eye)


def split_dot(ones, column):
    high = column.astype(jnp.bfloat16)
    rest = column - high.astype(jnp.float32)
    middle = rest.astype(jnp.bfloat16)
    low = (rest - middle.astype(jnp.float32)).astype(jnp.bfloat16)
    lane = lax.broadcasted_iota(jnp.int32, (column.shape[0], LANES), 1)
    parts = jnp.where(lane == 0, high.astype(jnp.float32), 0.0)
    parts = jnp.where(lane == 1, middle.astype(jnp.float32), parts)
    parts = jnp.where(lane == 2, low.astype(jnp.float32), parts).astype(jnp.bfloat16)
    summed = jnp.dot(ones, parts, preferred_element_type=jnp.float32)
    return jnp.sum(summed, axis=1, keepdims=True)


def attention(chunks, weight, out_weight, gain, collect, spread, unturn, width, group):
    pieces = len(chunks)
    samples, rows, length = chunks[0].shape
    channels = out_weight.shape[1]
    heads = channels // HEAD_DIM
    keys = pieces * length
    inner = length // width - 2

    def body(*refs):
        c_refs = refs[:pieces]
        w_ref, v_ref, g_ref, a_ref, b_ref, u_ref, o_ref, k_buf, v_buf = refs[pieces:]
        for i in range(samples):
            total = jnp.zeros((rows, 1), jnp.float32)
            for c in c_refs:
                total = total + jnp.sum(c[i].astype(jnp.float32), axis=1, keepdims=True)
            mean = split_dot(b_ref[...], split_dot(a_ref[...], total)) / (keys * group)
            total = jnp.zeros((rows, 1), jnp.float32)
            for c in c_refs:
                away = c[i].astype(jnp.float32) - mean
                total = total + jnp.sum(away * away, axis=1, keepdims=True)
            spread_of = split_dot(b_ref[...], split_dot(a_ref[...], total)) / (keys * group)
            scale = lax.rsqrt(spread_of + EPSILON) * g_ref[:, :1]
            for p, c in enumerate(c_refs):
                normed = ((c[i].astype(jnp.float32) - mean) * scale).astype(jnp.bfloat16)
                if p == 0:
                    queries = jnp.dot(
                        w_ref[:channels], normed, preferred_element_type=jnp.float32
                    ).astype(jnp.bfloat16)
                both = jnp.dot(
                    w_ref[channels:], normed, preferred_element_type=jnp.float32
                ).astype(jnp.bfloat16)
                k_buf[:, p * length : (p + 1) * length] = both[:channels]
                v_buf[:, p * length : (p + 1) * length] = both[channels:]
            queries = (queries.astype(jnp.float32) * HEAD_DIM ** (-0.5)).T.astype(jnp.bfloat16)
            own = c_refs[0][i].astype(jnp.float32).T.astype(jnp.bfloat16)
            summed = jnp.dot(own, u_ref[...], preferred_element_type=jnp.float32)
            for h in range(heads):
                cut = slice(h * HEAD_DIM, (h + 1) * HEAD_DIM)
                scores = jnp.dot(queries[:, cut], k_buf[cut], preferred_element_type=jnp.float32)
                shifted = jnp.exp(scores - jnp.max(scores, axis=1, keepdims=True))
                totals = jnp.sum(shifted, axis=1, keepdims=True)
                mixed = lax.dot_general(
                    shifted.astype(jnp.bfloat16), v_buf[cut], NT, preferred_element_type=jnp.float32
                )
                mixed = (mixed / totals).astype(jnp.bfloat16)
                summed = summed + jnp.dot(mixed, v_ref[cut], preferred_element_type=jnp.float32)
            result = summed.astype(jnp.bfloat16)
            o_ref[i, 0] = result[:width]
            o_ref[i, 1 + inner] = result[width : 2 * width]
            for r in range(inner):
                o_ref[i, 1 + r] = result[(2 + r) * width : (3 + r) * width]

    return call(
        body,
        jax.ShapeDtypeStruct((samples, length // width, width, channels), jnp.bfloat16),
        [pltpu.VMEM((channels, keys), jnp.bfloat16), pltpu.VMEM((channels, keys), jnp.bfloat16)],
    )(*chunks, weight, out_weight, gain, collect, spread, unturn)


def pad_rows(values, rows, axis):
    missing = rows - values.shape[axis]
    return jnp.pad(values, [(0, missing if a == axis else 0) for a in range(values.ndim)])


def local(
    features,
    step_index,
    roster,
    time_weight,
    temb_weight,
    norm_gains,
    conv_first,
    conv_second,
    attn_weight,
    out_weight,
):
    samples, height, width, channels = features.shape
    n, planes = lax.axis_size("fsdp"), lax.axis_size("spatial")
    mine, row = lax.axis_index("fsdp"), lax.axis_index("spatial")
    group = channels // GROUPS
    kept = conv_first.shape[1]
    shard = -(-kept // 16) * 16
    length = height * width
    entries = float(length * group)
    ends = jnp.stack([row > 0, row < planes - 1]).astype(jnp.int32)

    def ring(values):
        return [values] + [shift(values, "fsdp", j) for j in range(1, n)]

    def block(values, index, axis):
        return lax.dynamic_slice_in_dim(values, index % n * kept, kept, axis)

    flat = features.reshape(samples, length, channels)
    edges = ring(jnp.concatenate([flat[:, :width], flat[:, length - width :]], axis=1))
    mids = ring(flat[:, width : length - width])
    above = shift_rows(jnp.concatenate([e[:, width:] for e in edges], axis=0), 1)
    below = shift_rows(jnp.concatenate([e[:, :width] for e in edges], axis=0), -1)
    own_stats = local_stats(flat, same_group(channels, channels, channels, group), group)
    merged = merge_stats(lax.all_gather(own_stats, "spatial"), norm_gains[:1], entries)
    stats = ring(merged)

    taps = conv_first.reshape(3, 3, channels, kept).transpose(0, 1, 3, 2)
    first_weight = pad_rows(taps, shard, 2).reshape(3, 3 * shard, channels)
    taps = conv_second.reshape(3, 3, n, kept, kept)
    taps = jnp.stack(
        [lax.dynamic_index_in_dim(taps, (mine - j) % n, 2, keepdims=False) for j in range(n)], axis=2
    )
    taps = pad_rows(pad_rows(taps, shard, 3), shard, 4)
    second_weight = taps.transpose(0, 1, 4, 2, 3).reshape(3, 3 * shard, n * shard)
    bias = time_bias(step_index, roster, time_weight, block(temb_weight, mine, 1))
    bias = jnp.broadcast_to(pad_rows(bias, shard, 0)[:, None], (shard, LANES))
    index = jnp.arange(shard)
    pick = jnp.where(index < kept, index + mine * kept, -1)[:, None] == jnp.arange(channels)[None, :]
    count = n * samples
    eye = jnp.eye(2 * count, LANES, dtype=jnp.float32)

    edges, mids, own_stats, own_edges, own_mids = first_conv(
        ends,
        edges,
        mids,
        above,
        below,
        stats,
        first_weight,
        bias,
        same_group(shard, shard, kept, group),
        pick.astype(jnp.bfloat16),
        eye,
        width,
        group,
    )

    edges = ring(edges)
    mids = ring(mids)
    stacked = jnp.concatenate(edges, axis=0)
    above = shift_rows(stacked, 1)
    below = shift_rows(stacked, -1)
    gain = pad_rows(block(norm_gains[1:2], mine, 1), shard, 1)
    stats = ring(merge_stats(lax.all_gather(own_stats, "spatial"), gain, entries))
    sums = second_conv(
        ends,
        edges,
        mids,
        stats,
        above,
        below,
        second_weight,
        own_edges,
        own_mids,
        jnp.eye(shard, dtype=jnp.float32),
        samples,
        width,
    )

    own = jnp.concatenate([sums[0]] + [shift(sums[t], "fsdp", -t) for t in range(1, n)], axis=1)
    chunks = [own] + [shift(own, "spatial", 2 * d) for d in range(1, planes // 2)]
    swap = [(i, i ^ 1) for i in range(planes)]
    chunks = chunks + [lax.ppermute(c, "spatial", swap) for c in chunks]

    both = jnp.concatenate([attn_weight.T, out_weight.T], axis=0)
    part = both.shape[0] // planes
    both = lax.dynamic_slice_in_dim(both, row * part, part, 0).reshape(part, n, kept)

    def turned(values, to):
        order = [lax.dynamic_index_in_dim(values, (to + t) % n, 1, keepdims=False) for t in range(n)]
        return pad_rows(jnp.stack(order, axis=1), shard, 2).reshape(part, n * shard)

    gathered = jnp.stack(
        [turned(both, mine)] + [shift(turned(both, mine + j), "fsdp", j) for j in range(1, n)]
    )
    planes_of = [gathered] + [shift(gathered, "spatial", 2 * d) for d in range(1, planes // 2)]
    other = lax.ppermute(jnp.stack(planes_of), "spatial", swap)
    every = jnp.concatenate([jnp.stack(planes_of), other], axis=0)
    half = planes // 2
    ordered = []
    for s in range(planes):
        back = (row // 2 - s // 2) % half
        ordered.append(
            lax.dynamic_index_in_dim(every, back + half * ((row + s) % 2), 0, keepdims=False)
        )
    every = jnp.stack(ordered, axis=1).reshape(n, part * planes, n * shard)
    every = jnp.stack(
        [lax.dynamic_index_in_dim(every, (mine - g) % n, 0, keepdims=False) for g in range(n)]
    )
    qkv = every[:, : attn_weight.shape[1]].reshape(3 * channels, n * shard)
    unturned = every[:, attn_weight.shape[1] :].reshape(channels, n * shard)
    place = jnp.arange(n * shard)
    channel = (place // shard + mine) % n * kept + place % shard
    channel = jnp.where(place % shard < kept, channel, -1)
    unturn = (channel[:, None] == jnp.arange(channels)[None, :]).astype(jnp.bfloat16)
    last_weight = jnp.dot(unturned, unturn, preferred_element_type=jnp.float32).astype(jnp.bfloat16).T
    gain = jnp.concatenate(
        [pad_rows(block(norm_gains[2], mine + t, 0), shard, 0) for t in range(n)]
    )
    gain = jnp.broadcast_to(gain[:, None], (n * shard, LANES))
    groups_here = (place // shard * kept + place % shard) // group
    member = (groups_here[:, None] == jnp.arange(LANES)[None, :]) & (place % shard < kept)[:, None]
    spread = member.astype(jnp.bfloat16)
    return attention(chunks, qkv, last_weight, gain, spread.T, spread, unturn, width, group)


def shift_rows(values, step):
    count = lax.axis_size("spatial")
    pairs = [(i, i + step) for i in range(count) if 0 <= i + step < count]
    return lax.ppermute(values, "spatial", pairs)


def solution(mesh):
    in_specs = (
        P("fsdp", "spatial", None, None),
        P(),
        P(),
        P(),
        P(),
        P(),
        P(None, "fsdp"),
        P(None, "fsdp"),
        P(None, "fsdp"),
        P(None, "fsdp"),
    )
    out_specs = P("fsdp", "spatial", None, None)
    return jax.shard_map(local, mesh=mesh, in_specs=in_specs, out_specs=out_specs, check_vma=False)
```

```python
import math

import jax
import jax.numpy as jnp
import numpy as np
from jax import lax
from jax.experimental import pallas as pl
from jax.experimental.pallas import tpu as pltpu
from jax.sharding import PartitionSpec as P


HEAD_DIM = 64
GROUPS = 32
EPSILON = 1e-05
LANES = 128
HIGHEST = lax.Precision.HIGHEST


NT = (((1,), (1,)), ((), ()))


def call(body, out_shape, scratch=(), scalars=0, flops=0):
    def run(*operands):
        specs = [
            pl.BlockSpec(memory_space=pltpu.SMEM if i < scalars else pltpu.VMEM)
            for i in range(len(operands))
        ]
        outs = jax.tree.map(lambda _: pl.BlockSpec(memory_space=pltpu.VMEM), out_shape)
        return pl.pallas_call(
            body,
            out_shape=out_shape,
            in_specs=specs,
            out_specs=outs,
            scratch_shapes=list(scratch),
            compiler_params=pltpu.CompilerParams(vmem_limit_bytes=60 * 2**20),
            cost_estimate=pl.CostEstimate(flops=flops, transcendentals=0, bytes_accessed=0)
            if flops
            else None,
        )(*operands)

    return run


def shift(values, axis, step):
    count = lax.axis_size(axis)
    return lax.ppermute(values, axis, [(i, (i + step) % count) for i in range(count)])


def silu(v):
    half = 0.5 * v
    return half + half * jnp.tanh(half)


def time_bias(step_index, roster, time_weight, temb_columns, rows):
    freqs, hidden = time_weight.shape
    kept = temb_columns.shape[1]
    half_len = freqs // 2
    steps = roster.shape[0]

    def body(i_ref, r_ref, w_ref, t_ref, o_ref):
        at = lax.broadcasted_iota(jnp.int32, (1, steps), 1)
        moment = jnp.sum(jnp.where(at == i_ref[0], r_ref[...], 0.0), axis=1, keepdims=True)
        row = lax.broadcasted_iota(jnp.int32, (half_len, 1), 0).astype(jnp.float32)
        angles = moment * jnp.exp(-math.log(10000.0) * row / half_len)
        time_hidden = jnp.sum(jnp.cos(angles) * w_ref[:half_len], axis=0, keepdims=True) + jnp.sum(
            jnp.sin(angles) * w_ref[half_len:], axis=0, keepdims=True
        )
        time_hidden = time_hidden / (1.0 + jnp.exp(-time_hidden))
        parts = []
        for start in range(0, hidden, LANES):
            piece = jnp.broadcast_to(time_hidden[:, start : start + LANES], (LANES, LANES))
            parts.append(piece.T[:, :1] * t_ref[start : start + LANES])
        summed = jnp.sum(sum(parts[1:], parts[0]), axis=0, keepdims=True)
        o_ref[...] = jnp.zeros((rows, LANES), jnp.float32)
        for start in range(0, kept, LANES):
            size = min(LANES, kept - start)
            cut = summed[:, start : start + size]
            if size < LANES:
                cut = jnp.concatenate([cut, jnp.zeros((1, LANES - size), jnp.float32)], axis=1)
            turned = jnp.broadcast_to(cut, (LANES, LANES)).T
            o_ref[start : start + size] = turned[:size]

    return call(body, jax.ShapeDtypeStruct((rows, LANES), jnp.float32), scalars=1)(
        step_index, roster[None, :], time_weight, temb_columns
    )


def group_of(rows, block, kept, width):
    index = np.arange(rows)
    group = (index // block * kept + index % block) // width
    return np.where(index % block < kept, group, -1)


def members(rows, block, kept, width):
    group = group_of(rows, block, kept, width)[:, None]
    return jnp.asarray(group == np.arange(LANES)[None, :], jnp.bfloat16)


def same_group(rows, block, kept, width):
    group = group_of(rows, block, kept, width)[:, None]
    return jnp.asarray((group == group.T) & (group >= 0), jnp.float32)


def three_parts(values):
    high = values.astype(jnp.bfloat16).astype(jnp.float32)
    rest = values - high
    middle = rest.astype(jnp.bfloat16).astype(jnp.float32)
    return high, middle, rest - middle


def group_sums(row, member):
    for dims in ((((1,), (0,)), ((), ())), NT):
        at = lax.broadcasted_iota(jnp.int32, (8, row.shape[1]), 0)
        high, middle, low = three_parts(row)
        parts = jnp.where(at == 0, high, jnp.where(at == 1, middle, jnp.where(at == 2, low, 0.0)))
        summed = lax.dot_general(
            parts.astype(jnp.bfloat16), member, dims, preferred_element_type=jnp.float32
        )
        row = jnp.sum(summed, axis=0, keepdims=True)
    return row


def local_stats(features, member, width):
    samples, length, channels = features.shape

    def body(x_ref, g_ref, o_ref):
        for i in range(samples):
            v = x_ref[i].astype(jnp.float32)
            mean = group_sums(jnp.sum(v, axis=0, keepdims=True), g_ref[...]) / (length * width)
            c = v - mean
            o_ref[i : i + 1] = mean
            o_ref[samples + i : samples + i + 1] = group_sums(
                jnp.sum(c * c, axis=0, keepdims=True), g_ref[...]
            )

    return call(body, jax.ShapeDtypeStruct((2 * samples, channels), jnp.float32))(features, member)


def place(where, pieces, axis, flops=0):
    first = pieces[0]
    size = first.shape[axis]
    shape = list(first.shape)
    shape[axis] = size * len(pieces)

    def body(w_ref, *refs):
        for k, piece in enumerate(refs[:-1]):
            start = pl.multiple_of(w_ref[k] * size, size)
            refs[-1][(slice(None),) * axis + (pl.ds(start, size),)] = piece[...]

    return call(body, jax.ShapeDtypeStruct(tuple(shape), first.dtype), scalars=1, flops=flops)(
        where, *pieces
    )


def merge_stats(p_ref, gain, entries):
    devices, rows, _ = p_ref.shape
    count = rows // 2
    mean = p_ref[0, :count]
    for d in range(1, devices):
        mean = mean + p_ref[d, :count]
    mean = mean / devices
    squares = jnp.zeros_like(mean)
    for d in range(devices):
        away = p_ref[d, :count] - mean
        squares = squares + p_ref[d, count:] + entries * (away * away)
    return mean, lax.rsqrt(squares / (entries * devices) + EPSILON) * gain


TAIL = 16


def rows_message(parts, gain, entries, mids):
    samples, mid, channels = mids.shape

    def body(p_ref, g_ref, m_ref, o_ref):
        mean, scale = merge_stats(p_ref, g_ref[...], entries)
        for i in range(samples):
            o_ref[i, :mid] = m_ref[i]
            rows = [*three_parts(mean[i : i + 1]), *three_parts(scale[i : i + 1])]
            rows.append(jnp.zeros((TAIL - len(rows), channels), jnp.float32))
            o_ref[i, mid:] = jnp.concatenate(rows, axis=0).astype(jnp.bfloat16)

    shape = jax.ShapeDtypeStruct((samples, mid + TAIL, channels), jnp.bfloat16)
    return call(body, shape)(parts, gain, mids)


def columns_message(parts, gain, entries, mids):
    shard, wide = mids.shape

    def body(p_ref, g_ref, m_ref, o_ref):
        o_ref[:, :wide] = m_ref[...]
        figures = jnp.concatenate(merge_stats(p_ref, g_ref[...], entries), axis=0)
        rows = [*three_parts(figures)]
        rows.append(jnp.zeros((LANES - 3 * figures.shape[0], shard), jnp.float32))
        rows = jnp.concatenate(rows, axis=0).astype(jnp.bfloat16)
        o_ref[:, wide:] = lax.dot_general(
            identity(shard, shard), rows, NT, preferred_element_type=jnp.float32
        ).astype(jnp.bfloat16)

    shape = jax.ShapeDtypeStruct((shard, wide + LANES), jnp.bfloat16)
    return call(body, shape)(parts, gain, mids)


def identity(rows, columns):
    at = lax.broadcasted_iota(jnp.int32, (rows, columns), 0)
    same = at == lax.broadcasted_iota(jnp.int32, (rows, columns), 1)
    return jnp.where(same, 1.0, 0.0).astype(jnp.bfloat16)


def tap_rows(weight, row, depth):
    return jnp.concatenate(
        [weight[:, (3 * row + b) * depth : (3 * row + b + 1) * depth] for b in range(3)], axis=0
    )


def pick_column(values, at, period):
    lane = lax.broadcasted_iota(jnp.int32, values.shape, 1)
    chosen = (lane == at) | (lane == at + period) | (lane == at + 2 * period)
    return jnp.sum(jnp.where(chosen, values, 0.0), axis=1, keepdims=True)


def column_shift(y, shard, width):
    lane = lax.broadcasted_iota(jnp.int32, (shard, LANES), 1) % width
    tiles = []
    for start in range(0, y.shape[1], LANES):
        left = y[:shard, start : start + LANES]
        right = y[2 * shard :, start : start + LANES]
        tiles.append(
            y[shard : 2 * shard, start : start + LANES]
            + jnp.where(lane > 0, pltpu.roll(left, 1, axis=1), 0.0)
            + jnp.where(lane < width - 1, pltpu.roll(right, LANES - 1, axis=1), 0.0)
        )
    return jnp.concatenate(tiles, axis=1)


def first_conv(ends, edges, mids, above, below, weight, bias, groups, pick, eye, width, group):
    n = len(edges)
    samples, edge, channels = edges[0].shape
    mid = mids[0].shape[1] - TAIL
    shard = bias.shape[0]
    count = n * samples
    inner = mid // width
    length = edge + mid

    def body(*refs):
        ends_ref = refs[0]
        e_refs, m_refs = refs[1 : 1 + n], refs[1 + n : 1 + 2 * n]
        a_ref, b_ref, w_ref, t_ref, g_ref, p_ref, i_ref = refs[1 + 2 * n : 8 + 2 * n]
        eo_ref, mo_ref, so_ref, fe_ref, fm_ref, buf, out_buf = refs[8 + 2 * n :]
        has_above = ends_ref[0].astype(jnp.float32)
        has_below = ends_ref[1].astype(jnp.float32)
        lane = lax.broadcasted_iota(jnp.int32, (shard, LANES), 1)
        sums = jnp.zeros((shard, LANES), jnp.float32)
        for j in range(n):
            for i in range(samples):
                q = j * samples + i
                tail = m_refs[j][i, mid:].astype(jnp.float32)
                mean = tail[0:1] + tail[1:2] + tail[2:3]
                scale = tail[3:4] + tail[4:5] + tail[5:6]

                def act(x):
                    return silu((x.astype(jnp.float32) - mean) * scale)

                e = e_refs[j][i]
                m = m_refs[j][i, :mid]
                ea = act(e).astype(jnp.bfloat16)
                buf[:width] = (act(a_ref[q]) * has_above).astype(jnp.bfloat16)
                buf[width : 2 * width] = ea[:width]
                buf[2 * width : 2 * width + mid] = act(m).astype(jnp.bfloat16)
                buf[2 * width + mid : 3 * width + mid] = ea[width:]
                buf[3 * width + mid :] = (act(b_ref[q]) * has_below).astype(jnp.bfloat16)
                y = jnp.zeros((3 * shard, length), jnp.float32)
                for a in range(3):
                    window = jnp.concatenate(
                        [
                            buf[a * width : (a + 1) * width],
                            buf[(a + 1 + inner) * width : (a + 2 + inner) * width],
                            buf[(a + 1) * width : (a + 1 + inner) * width],
                        ],
                        axis=0,
                    )
                    y = y + lax.dot_general(
                        tap_rows(w_ref, a, channels), window, NT, preferred_element_type=jnp.float32
                    )
                out = column_shift(y, shard, width) + t_ref[:, :1]
                eo_ref[:, q * edge : (q + 1) * edge] = out[:, :edge].astype(jnp.bfloat16)
                mo_ref[:, q * mid : (q + 1) * mid] = out[:, edge:].astype(jnp.bfloat16)
                fe_ref[:, q * edge : (q + 1) * edge] = lax.dot_general(
                    p_ref[...], e, NT, preferred_element_type=jnp.float32
                ).astype(jnp.bfloat16)
                fm_ref[:, q * mid : (q + 1) * mid] = lax.dot_general(
                    p_ref[...], m, NT, preferred_element_type=jnp.float32
                ).astype(jnp.bfloat16)
                out_buf[q] = out
                sums = jnp.where(lane == q, jnp.sum(out, axis=1, keepdims=True), sums)
        centers = jnp.dot(g_ref[...], sums, precision=HIGHEST) / (length * group)
        sums = jnp.zeros((shard, LANES), jnp.float32)
        for q in range(count):
            c = out_buf[q] - centers[:, q : q + 1]
            sums = jnp.where(lane == q, jnp.sum(c * c, axis=1, keepdims=True), sums)
        squares = jnp.dot(g_ref[...], sums, precision=HIGHEST)
        for start, found in ((0, centers), (count, squares)):
            so_ref[start : start + count] = lax.dot_general(
                i_ref[...], found, NT, precision=HIGHEST
            )[:count]

    out_shape = (
        jax.ShapeDtypeStruct((shard, count * edge), jnp.bfloat16),
        jax.ShapeDtypeStruct((shard, count * mid), jnp.bfloat16),
        jax.ShapeDtypeStruct((2 * count, shard), jnp.float32),
        jax.ShapeDtypeStruct((shard, count * edge), jnp.bfloat16),
        jax.ShapeDtypeStruct((shard, count * mid), jnp.bfloat16),
    )
    scratch = [
        pltpu.VMEM((length + 2 * width, channels), jnp.bfloat16),
        pltpu.VMEM((count, shard, length), jnp.float32),
    ]
    return call(body, out_shape, scratch, scalars=1, flops=6 * count * length * channels * 3 * shard)(
        ends, *edges, *mids, above, below, weight, bias, groups, pick, eye
    )


def second_conv(ends, edges, mids, above, below, weight, own_edges, own_mids, samples, width):
    n = len(edges)
    shard = edges[0].shape[0]
    count = n * samples
    edge, mid = edges[0].shape[1] // count, (mids[0].shape[1] - LANES) // count
    length = edge + mid

    def body(*refs):
        ends_ref = refs[0]
        e_refs, m_refs = refs[1 : 1 + n], refs[1 + n : 1 + 2 * n]
        a_ref, b_ref, w_ref, fe_ref, fm_ref = refs[1 + 2 * n : 6 + 2 * n]
        o_ref, buf = refs[6 + 2 * n :]
        has_above = ends_ref[0].astype(jnp.float32)
        has_below = ends_ref[1].astype(jnp.float32)
        lane = lax.broadcasted_iota(jnp.int32, (shard, LANES), 1)
        low = lane < width
        columns = [m_refs[j][:, count * mid :].astype(jnp.float32) for j in range(n)]

        def sample(t, i):
            for j in range(n):
                q = lax.rem(t - j + n, n) * samples + i
                mean, scale = (pick_column(columns[j], at, 2 * count) for at in (q, count + q))

                def act(x):
                    return silu((x.astype(jnp.float32) - mean) * scale)

                rows = slice(j * shard, (j + 1) * shard)
                natural = pl.ds(pl.multiple_of(lax.rem(ends_ref[2] + n - j, n) * shard, 16), shard)
                cut = pl.ds(pl.multiple_of(q * edge, LANES), edge)
                e = act(e_refs[j][:, cut])
                m = act(m_refs[j][:, pl.ds(pl.multiple_of(q * mid, LANES), mid)])
                top = pltpu.roll(act(a_ref[rows, cut]), width, axis=1) * has_above
                bottom = pltpu.roll(act(b_ref[rows, cut]), width, axis=1) * has_below
                turned = pltpu.roll(m, width, axis=1)
                buf[0, natural, :edge] = jnp.where(low, top, m).astype(jnp.bfloat16)
                buf[0, natural, edge:] = jnp.where(low, e, turned).astype(jnp.bfloat16)
                buf[1, natural, :edge] = e.astype(jnp.bfloat16)
                buf[1, natural, edge:] = m.astype(jnp.bfloat16)
                buf[2, natural, :edge] = jnp.where(low, m, bottom).astype(jnp.bfloat16)
                buf[2, natural, edge:] = jnp.where(low, turned, e).astype(jnp.bfloat16)
            y = jnp.zeros((3 * shard, length), jnp.float32)
            for a in range(3):
                y = y + jnp.dot(
                    tap_rows(w_ref, a, n * shard), buf[a], preferred_element_type=jnp.float32
                )
            out = column_shift(y, shard, width)
            q = t * samples + i
            cut = pl.ds(pl.multiple_of(q * edge, LANES), edge)
            o_ref[t, i, :, :edge] = (out[:, :edge] + fe_ref[:, cut].astype(jnp.float32)).astype(
                jnp.bfloat16
            )
            cut = pl.ds(pl.multiple_of(q * mid, LANES), mid)
            o_ref[t, i, :, edge:] = (out[:, edge:] + fm_ref[:, cut].astype(jnp.float32)).astype(
                jnp.bfloat16
            )

        @pl.loop(0, n)
        def _(t):
            for i in range(samples):
                sample(t, i)

    return call(
        body,
        jax.ShapeDtypeStruct((n, samples, shard, length), jnp.bfloat16),
        [pltpu.VMEM((3, n * shard, length), jnp.bfloat16)],
        scalars=1,
        flops=6 * count * length * n * shard * 3 * shard,
    )(ends, *edges, *mids, above, below, weight, own_edges, own_mids)


def split_dot(ones, column):
    high = column.astype(jnp.bfloat16)
    rest = column - high.astype(jnp.float32)
    middle = rest.astype(jnp.bfloat16)
    low = (rest - middle.astype(jnp.float32)).astype(jnp.bfloat16)
    lane = lax.broadcasted_iota(jnp.int32, (column.shape[0], LANES), 1)
    parts = jnp.where(lane == 0, high.astype(jnp.float32), 0.0)
    parts = jnp.where(lane == 1, middle.astype(jnp.float32), parts)
    parts = jnp.where(lane == 2, low.astype(jnp.float32), parts).astype(jnp.bfloat16)
    summed = jnp.dot(ones, parts, preferred_element_type=jnp.float32)
    return jnp.sum(summed, axis=1, keepdims=True)


def attention(chunks, weights, out_weight, gain, spread, unpad, used, width, group):
    pieces = len(chunks)
    samples, rows, length = chunks[0].shape
    channels = gain.shape[0] if unpad is None else unpad.shape[1]
    heads = channels // HEAD_DIM
    keys = pieces * length
    inner = length // width - 2
    blocks = weights.shape[0]

    def body(*refs):
        c_refs = refs[:pieces]
        w_ref, g_ref, a_ref, b_ref = refs[pieces : pieces + 4]
        v_ref = None if out_weight is None else refs[-5]
        o_ref, buf, query_buf, mixed_buf = refs[-4:]
        for i in range(samples):
            total = jnp.zeros((rows, 1), jnp.float32)
            for c in c_refs:
                total = total + jnp.sum(c[i].astype(jnp.float32), axis=1, keepdims=True)
            mean = split_dot(b_ref[...], split_dot(a_ref[...], total)) / (keys * group)
            total = jnp.zeros((rows, 1), jnp.float32)
            for c in c_refs:
                away = c[i].astype(jnp.float32) - mean
                total = total + jnp.sum(away * away, axis=1, keepdims=True)
            spread_of = split_dot(b_ref[...], split_dot(a_ref[...], total)) / (keys * group)
            scale = lax.rsqrt(spread_of + EPSILON) * g_ref[:, :1]
            for p, c in enumerate(c_refs):
                normed = ((c[i].astype(jnp.float32) - mean) * scale).astype(jnp.bfloat16)
                for g in range(blocks):
                    low = max(0, (0 if p == 0 else channels) - g * used)
                    if low < used:
                        buf[g * used + low : (g + 1) * used, p * length : (p + 1) * length] = jnp.dot(
                            w_ref[g, low:used], normed, preferred_element_type=jnp.float32
                        ).astype(jnp.bfloat16)
            queries = buf[:channels, :length].astype(jnp.float32) * HEAD_DIM ** (-0.5)
            query_buf[...] = queries.T.astype(jnp.bfloat16)

            @pl.loop(0, heads // 2)
            def _(two):
                lanes = pl.ds(pl.multiple_of(two * LANES, LANES), LANES)
                at = channels + two * LANES
                k_two = buf[pl.ds(pl.multiple_of(at, LANES), LANES)]
                v_two = buf[pl.ds(pl.multiple_of(at + channels, LANES), LANES)]
                q_two = query_buf[:, lanes]
                pair = []
                for h in range(2):
                    cut = slice(h * HEAD_DIM, (h + 1) * HEAD_DIM)
                    scores = jnp.dot(q_two[:, cut], k_two[cut], preferred_element_type=jnp.float32)
                    shifted = jnp.exp(scores - jnp.max(scores, axis=1, keepdims=True))
                    totals = jnp.sum(shifted, axis=1, keepdims=True)
                    mixed = lax.dot_general(
                        shifted.astype(jnp.bfloat16),
                        v_two[cut],
                        NT,
                        preferred_element_type=jnp.float32,
                    )
                    pair.append(mixed / totals)
                mixed_buf[:, lanes] = jnp.concatenate(pair, axis=1).astype(jnp.bfloat16)

            own = c_refs[0][i].astype(jnp.float32).T
            if unpad is not None:
                own = jnp.dot(
                    own.astype(jnp.bfloat16), refs[pieces + 4][...], preferred_element_type=jnp.float32
                )
            if out_weight is None:
                kept = channels // blocks
                v_rows = [w_ref[g, used : used + kept] for g in range(blocks)]
                v_rows = jnp.concatenate(v_rows, axis=0)
            else:
                v_rows = v_ref[...]
            result = own + lax.dot_general(
                mixed_buf[...], v_rows, NT, preferred_element_type=jnp.float32
            )
            result = result.astype(jnp.bfloat16)
            o_ref[i, 0] = result[:width]
            o_ref[i, 1 + inner] = result[width : 2 * width]
            for r in range(inner):
                o_ref[i, 1 + r] = result[(2 + r) * width : (3 + r) * width]

    operands = [*chunks, weights, gain, spread.T, spread]
    if unpad is not None:
        operands.append(unpad)
    if out_weight is not None:
        operands.append(out_weight)
    return call(
        body,
        jax.ShapeDtypeStruct((samples, length // width, width, channels), jnp.bfloat16),
        [
            pltpu.VMEM((3 * channels, keys), jnp.bfloat16),
            pltpu.VMEM((length, channels), jnp.bfloat16),
            pltpu.VMEM((length, channels), jnp.bfloat16),
        ],
    )(*operands)


def pad_rows(values, rows, axis):
    missing = rows - values.shape[axis]
    return jnp.pad(values, [(0, missing if a == axis else 0) for a in range(values.ndim)])


def local(
    features,
    step_index,
    roster,
    time_weight,
    temb_weight,
    norm_gains,
    conv_first,
    conv_second,
    attn_weight,
    out_weight,
):
    samples, height, width, channels = features.shape
    n, planes = lax.axis_size("fsdp"), lax.axis_size("spatial")
    mine, row = lax.axis_index("fsdp"), lax.axis_index("spatial")
    group = channels // GROUPS
    kept = conv_first.shape[1]
    shard = -(-kept // 16) * 16
    length = height * width
    entries = float(length * group)
    count = n * samples
    half = planes // 2
    swap = [(i, i ^ 1) for i in range(planes)]
    ends = jnp.stack([row > 0, row < planes - 1, mine]).astype(jnp.int32)

    def ring(values):
        return [values] + [shift(values, "fsdp", j) for j in range(1, n)]

    def block(values, axis):
        return lax.dynamic_slice_in_dim(values, mine * kept, kept, axis)

    def pad_blocks(values, axis):
        if shard == kept:
            return values
        shape = list(values.shape)
        parts = values.reshape(shape[:axis] + [shape[axis] // kept, kept] + shape[axis + 1 :])
        parts = pad_rows(parts, shard, axis + 1)
        return parts.reshape(shape[:axis] + [shape[axis] // kept * shard] + shape[axis + 1 :])

    def in_plane_stats(values):
        values = values[None]
        size = 1
        while size < planes:
            other = lax.ppermute(values, "spatial", [(i, i ^ size) for i in range(planes)])
            values = jnp.concatenate([values, other], axis=0)
            size *= 2
        return values

    def in_plane(values):
        near = [values] + [shift(values, "spatial", 2 * d) for d in range(1, half)]
        far = [lax.ppermute(c, "spatial", swap) for c in near]
        back = (row - 2 * np.arange(half)) % planes
        return near + far, jnp.concatenate([back, back ^ 1]).astype(jnp.int32)

    flat = features.reshape(samples, length, channels)
    own_stats = local_stats(flat, members(channels, channels, channels, group), group)
    edges = ring(jnp.concatenate([flat[:, :width], flat[:, length - width :]], axis=1))
    above = shift_rows(jnp.concatenate([e[:, width:] for e in edges], axis=0), 1)
    below = shift_rows(jnp.concatenate([e[:, :width] for e in edges], axis=0), -1)
    own_stats = in_plane_stats(own_stats)
    mids = rows_message(own_stats, norm_gains[:1], entries, flat[:, width : length - width])
    mids = ring(mids)

    wide = attn_weight.shape[1]
    part = -(-(wide + kept) // (16 * planes)) * 16
    turned = jnp.concatenate(
        [pad_blocks(attn_weight.T, 1), pad_rows(out_weight.T, n * shard, 1)], axis=0
    )
    turned = lax.dynamic_slice_in_dim(pad_rows(turned, part * planes, 0), row * part, part, 0)
    turned = lax.all_gather(turned, ("fsdp", "spatial"), axis=0)
    turned = turned.reshape(n, planes * part, n * shard)

    projection, used, last_weight = turned, wide, None
    if shard != kept:
        projection = turned[:, :wide].reshape(1, n * wide, n * shard)
        used = n * wide
        last_weight = turned[:, wide : wide + kept, :channels].reshape(channels, channels)
    first_weight = pad_rows(conv_first.T, shard, 0)
    second_weight = pad_rows(pad_blocks(conv_second.T, 1), shard, 0)
    bias = time_bias(step_index, roster, time_weight, block(temb_weight, 1), shard)
    index = jnp.arange(shard)
    pick = jnp.where(index < kept, index + mine * kept, -1)[:, None] == jnp.arange(channels)[None, :]

    edges, mids, own_stats, own_edges, own_mids = first_conv(
        ends,
        edges,
        mids,
        above,
        below,
        first_weight,
        bias,
        same_group(shard, shard, kept, group),
        pick.astype(jnp.bfloat16),
        jnp.asarray(np.eye(-(-count // 8) * 8, LANES, dtype=np.float32)),
        width,
        group,
    )

    edges = ring(edges)
    stacked = jnp.concatenate(edges, axis=0)
    above = shift_rows(stacked, 1)
    below = shift_rows(stacked, -1)
    gain = pad_rows(block(norm_gains[1:2], 1), shard, 1)
    own_stats = in_plane_stats(own_stats)
    mids = columns_message(own_stats, gain, entries, mids)
    mids = ring(mids)
    sums = second_conv(
        ends,
        edges,
        mids,
        above,
        below,
        second_weight,
        own_edges,
        own_mids,
        samples,
        width,
    )

    own = [sums[0]] + [shift(sums[t], "fsdp", -t) for t in range(1, n)]
    own = place(((mine + np.arange(n)) % n).astype(jnp.int32), own, 1)
    chunks, _ = in_plane(own)
    gain = jnp.broadcast_to(pad_blocks(norm_gains[2], 0)[:, None], (n * shard, LANES))
    unpad = None
    if shard != kept:
        at = np.arange(n * shard)
        at = np.where(at % shard < kept, at // shard * kept + at % shard, -1)
        unpad = jnp.asarray(at[:, None] == np.arange(channels)[None, :], jnp.bfloat16)
    return attention(
        chunks,
        projection,
        last_weight,
        gain,
        members(n * shard, shard, kept, group),
        unpad,
        used,
        width,
        group,
    )


def shift_rows(values, step):
    count = lax.axis_size("spatial")
    pairs = [(i, i + step) for i in range(count) if 0 <= i + step < count]
    return lax.ppermute(values, "spatial", pairs)


def solution(mesh):
    in_specs = (
        P("fsdp", "spatial", None, None),
        P(),
        P(),
        P(),
        P(),
        P(),
        P(None, "fsdp"),
        P(None, "fsdp"),
        P(None, "fsdp"),
        P(None, "fsdp"),
    )
    out_specs = P("fsdp", "spatial", None, None)

    return jax.shard_map(local, mesh=mesh, in_specs=in_specs, out_specs=out_specs, check_vma=False)
```

```python
import math

import jax
import jax.numpy as jnp
import numpy as np
from jax import lax
from jax.experimental import pallas as pl
from jax.experimental.pallas import tpu as pltpu
from jax.sharding import PartitionSpec as P


HEAD_DIM = 64
GROUPS = 32
EPSILON = 1e-05
LANES = 128
HIGHEST = lax.Precision.HIGHEST


NT = (((1,), (1,)), ((), ()))


def call(body, out_shape, scratch=(), scalars=0, flops=0):
    def run(*operands):
        specs = [
            pl.BlockSpec(memory_space=pltpu.SMEM if i < scalars else pltpu.VMEM)
            for i in range(len(operands))
        ]
        outs = jax.tree.map(lambda _: pl.BlockSpec(memory_space=pltpu.VMEM), out_shape)
        return pl.pallas_call(
            body,
            out_shape=out_shape,
            in_specs=specs,
            out_specs=outs,
            scratch_shapes=list(scratch),
            compiler_params=pltpu.CompilerParams(vmem_limit_bytes=60 * 2**20),
            cost_estimate=pl.CostEstimate(flops=flops, transcendentals=0, bytes_accessed=0)
            if flops
            else None,
        )(*operands)

    return run


def shift(values, axis, step):
    count = lax.axis_size(axis)
    return lax.ppermute(values, axis, [(i, (i + step) % count) for i in range(count)])


def silu(v):
    half = 0.5 * v
    return half + half * jnp.tanh(half)


def time_bias(step_index, roster, time_weight, temb_columns, rows):
    freqs, hidden = time_weight.shape
    kept = temb_columns.shape[1]
    half_len = freqs // 2
    steps = roster.shape[0]

    def body(i_ref, r_ref, w_ref, t_ref, o_ref):
        at = lax.broadcasted_iota(jnp.int32, (1, steps), 1)
        moment = jnp.sum(jnp.where(at == i_ref[0], r_ref[...], 0.0), axis=1, keepdims=True)
        row = lax.broadcasted_iota(jnp.int32, (half_len, 1), 0).astype(jnp.float32)
        angles = moment * jnp.exp(-math.log(10000.0) * row / half_len)
        time_hidden = jnp.sum(jnp.cos(angles) * w_ref[:half_len], axis=0, keepdims=True) + jnp.sum(
            jnp.sin(angles) * w_ref[half_len:], axis=0, keepdims=True
        )
        time_hidden = time_hidden / (1.0 + jnp.exp(-time_hidden))
        parts = []
        for start in range(0, hidden, LANES):
            piece = jnp.broadcast_to(time_hidden[:, start : start + LANES], (LANES, LANES))
            parts.append(piece.T[:, :1] * t_ref[start : start + LANES])
        summed = jnp.sum(sum(parts[1:], parts[0]), axis=0, keepdims=True)
        o_ref[...] = jnp.zeros((rows, LANES), jnp.float32)
        for start in range(0, kept, LANES):
            size = min(LANES, kept - start)
            cut = summed[:, start : start + size]
            if size < LANES:
                cut = jnp.concatenate([cut, jnp.zeros((1, LANES - size), jnp.float32)], axis=1)
            turned = jnp.broadcast_to(cut, (LANES, LANES)).T
            o_ref[start : start + size] = turned[:size]

    return call(body, jax.ShapeDtypeStruct((rows, LANES), jnp.float32), scalars=1)(
        step_index, roster[None, :], time_weight, temb_columns
    )


def group_of(rows, block, kept, width):
    index = np.arange(rows)
    group = (index // block * kept + index % block) // width
    return np.where(index % block < kept, group, -1)


def members(rows, block, kept, width):
    group = group_of(rows, block, kept, width)[:, None]
    return jnp.asarray(group == np.arange(LANES)[None, :], jnp.bfloat16)


def same_group(rows, block, kept, width):
    group = group_of(rows, block, kept, width)[:, None]
    return jnp.asarray((group == group.T) & (group >= 0), jnp.float32)


def three_parts(values):
    high = values.astype(jnp.bfloat16).astype(jnp.float32)
    rest = values - high
    middle = rest.astype(jnp.bfloat16).astype(jnp.float32)
    return high, middle, rest - middle


def group_sums(row, member):
    for dims in ((((1,), (0,)), ((), ())), NT):
        at = lax.broadcasted_iota(jnp.int32, (8, row.shape[1]), 0)
        high, middle, low = three_parts(row)
        parts = jnp.where(at == 0, high, jnp.where(at == 1, middle, jnp.where(at == 2, low, 0.0)))
        summed = lax.dot_general(
            parts.astype(jnp.bfloat16), member, dims, preferred_element_type=jnp.float32
        )
        row = jnp.sum(summed, axis=0, keepdims=True)
    return row


def local_stats(features, member, width):
    samples, length, channels = features.shape

    def body(x_ref, g_ref, o_ref):
        for i in range(samples):
            v = x_ref[i].astype(jnp.float32)
            mean = group_sums(jnp.sum(v, axis=0, keepdims=True), g_ref[...]) / (length * width)
            c = v - mean
            o_ref[i : i + 1] = mean
            o_ref[samples + i : samples + i + 1] = group_sums(
                jnp.sum(c * c, axis=0, keepdims=True), g_ref[...]
            )

    return call(body, jax.ShapeDtypeStruct((2 * samples, channels), jnp.float32))(features, member)


def place(where, pieces, axis, flops=0):
    first = pieces[0]
    size = first.shape[axis]
    shape = list(first.shape)
    shape[axis] = size * len(pieces)

    def body(w_ref, *refs):
        for k, piece in enumerate(refs[:-1]):
            start = pl.multiple_of(w_ref[k] * size, size)
            refs[-1][(slice(None),) * axis + (pl.ds(start, size),)] = piece[...]

    return call(body, jax.ShapeDtypeStruct(tuple(shape), first.dtype), scalars=1, flops=flops)(
        where, *pieces
    )


def merge_stats(p_ref, gain, entries):
    devices, rows, _ = p_ref.shape
    count = rows // 2
    mean = p_ref[0, :count]
    for d in range(1, devices):
        mean = mean + p_ref[d, :count]
    mean = mean / devices
    squares = jnp.zeros_like(mean)
    for d in range(devices):
        away = p_ref[d, :count] - mean
        squares = squares + p_ref[d, count:] + entries * (away * away)
    return mean, lax.rsqrt(squares / (entries * devices) + EPSILON) * gain


TAIL = 16


def rows_message(parts, gain, entries, mids):
    samples, mid, channels = mids.shape

    def body(p_ref, g_ref, m_ref, o_ref):
        mean, scale = merge_stats(p_ref, g_ref[...], entries)
        for i in range(samples):
            o_ref[i, :mid] = m_ref[i]
            rows = [*three_parts(mean[i : i + 1]), *three_parts(scale[i : i + 1])]
            rows.append(jnp.zeros((TAIL - len(rows), channels), jnp.float32))
            o_ref[i, mid:] = jnp.concatenate(rows, axis=0).astype(jnp.bfloat16)

    shape = jax.ShapeDtypeStruct((samples, mid + TAIL, channels), jnp.bfloat16)
    return call(body, shape)(parts, gain, mids)


def columns_message(parts, gain, entries, mids):
    shard, wide = mids.shape

    def body(p_ref, g_ref, m_ref, o_ref):
        o_ref[:, :wide] = m_ref[...]
        figures = jnp.concatenate(merge_stats(p_ref, g_ref[...], entries), axis=0)
        rows = [*three_parts(figures)]
        rows.append(jnp.zeros((LANES - 3 * figures.shape[0], shard), jnp.float32))
        rows = jnp.concatenate(rows, axis=0).astype(jnp.bfloat16)
        o_ref[:, wide:] = lax.dot_general(
            identity(shard, shard), rows, NT, preferred_element_type=jnp.float32
        ).astype(jnp.bfloat16)

    shape = jax.ShapeDtypeStruct((shard, wide + LANES), jnp.bfloat16)
    return call(body, shape)(parts, gain, mids)


def identity(rows, columns):
    at = lax.broadcasted_iota(jnp.int32, (rows, columns), 0)
    same = at == lax.broadcasted_iota(jnp.int32, (rows, columns), 1)
    return jnp.where(same, 1.0, 0.0).astype(jnp.bfloat16)


def halo_rows(edges, width):
    samples, _, channels = edges[0].shape
    shape = jax.ShapeDtypeStruct((len(edges) * samples, width, channels), jnp.bfloat16)

    def body(*refs):
        for j, e in enumerate(refs[:-2]):
            refs[-2][j * samples : (j + 1) * samples] = e[:, width:]
            refs[-1][j * samples : (j + 1) * samples] = e[:, :width]

    return call(body, (shape, shape))(*edges)


def halo_columns(edges, width):
    shard, wide = edges[0].shape
    edge = 2 * width
    shape = jax.ShapeDtypeStruct((len(edges) * shard, wide // 2), jnp.bfloat16)

    def body(*refs):
        low = lax.broadcasted_iota(jnp.int32, (shard, edge), 1) < width
        for j, e in enumerate(refs[:-2]):
            rows = slice(j * shard, (j + 1) * shard)
            for p in range(wide // edge // 2):
                left = e[:, 2 * p * edge : (2 * p + 1) * edge].astype(jnp.float32)
                right = e[:, (2 * p + 1) * edge : (2 * p + 2) * edge].astype(jnp.float32)
                cut = slice(p * edge, (p + 1) * edge)
                last = jnp.where(low, pltpu.roll(left, width, axis=1), right)
                first = jnp.where(low, left, pltpu.roll(right, width, axis=1))
                refs[-2][rows, cut] = last.astype(jnp.bfloat16)
                refs[-1][rows, cut] = first.astype(jnp.bfloat16)

    return call(body, (shape, shape))(*edges)


def tap_rows(weight, row, depth):
    return jnp.concatenate(
        [weight[:, (3 * row + b) * depth : (3 * row + b + 1) * depth] for b in range(3)], axis=0
    )


def spread_column(tail, at, period):
    lane = lax.broadcasted_iota(jnp.int32, (LANES, LANES), 0)
    chosen = (lane == at) | (lane == at + period) | (lane == at + 2 * period)
    chosen = jnp.where(chosen, 1.0, 0.0).astype(jnp.bfloat16)
    return jnp.dot(tail, chosen, preferred_element_type=jnp.float32)


def tile(index, size):
    if isinstance(index, int):
        return slice(index * size, (index + 1) * size)
    return pl.ds(pl.multiple_of(index * size, LANES), size)


def column_shift(y, shard, width):
    lane = lax.broadcasted_iota(jnp.int32, (shard, LANES), 1) % width
    tiles = []
    for start in range(0, y.shape[1], LANES):
        left = y[:shard, start : start + LANES]
        right = y[2 * shard :, start : start + LANES]
        tiles.append(
            y[shard : 2 * shard, start : start + LANES]
            + jnp.where(lane > 0, pltpu.roll(left, 1, axis=1), 0.0)
            + jnp.where(lane < width - 1, pltpu.roll(right, LANES - 1, axis=1), 0.0)
        )
    return jnp.concatenate(tiles, axis=1)


def first_conv(ends, edges, mids, above, below, weight, bias, groups, pick, eye, width, group):
    n = len(edges)
    samples, edge, channels = edges[0].shape
    mid = mids[0].shape[1] - TAIL
    shard = bias.shape[0]
    count = n * samples
    inner = mid // width
    length = edge + mid

    def body(*refs):
        ends_ref = refs[0]
        e_refs, m_refs = refs[1 : 1 + n], refs[1 + n : 1 + 2 * n]
        a_ref, b_ref, w_ref, t_ref, g_ref, p_ref, i_ref = refs[1 + 2 * n : 8 + 2 * n]
        eo_ref, mo_ref, so_ref, fe_ref, fm_ref, buf, out_buf = refs[8 + 2 * n :]
        has_above = ends_ref[0].astype(jnp.float32)
        has_below = ends_ref[1].astype(jnp.float32)
        lane = lax.broadcasted_iota(jnp.int32, (shard, LANES), 1)
        sums = jnp.zeros((shard, LANES), jnp.float32)
        for j in range(n):
            for i in range(samples):
                q = j * samples + i
                tail = m_refs[j][i, mid:].astype(jnp.float32)
                mean = tail[0:1] + tail[1:2] + tail[2:3]
                scale = tail[3:4] + tail[4:5] + tail[5:6]

                def act(x):
                    return silu((x.astype(jnp.float32) - mean) * scale)

                e = e_refs[j][i]
                m = m_refs[j][i, :mid]
                ea = act(e).astype(jnp.bfloat16)
                buf[:width] = (act(a_ref[q]) * has_above).astype(jnp.bfloat16)
                buf[width : 2 * width] = ea[:width]
                buf[2 * width : 2 * width + mid] = act(m).astype(jnp.bfloat16)
                buf[2 * width + mid : 3 * width + mid] = ea[width:]
                buf[3 * width + mid :] = (act(b_ref[q]) * has_below).astype(jnp.bfloat16)
                y = jnp.zeros((3 * shard, length), jnp.float32)
                for a in range(3):
                    window = jnp.concatenate(
                        [
                            buf[a * width : (a + 1) * width],
                            buf[(a + 1 + inner) * width : (a + 2 + inner) * width],
                            buf[(a + 1) * width : (a + 1 + inner) * width],
                        ],
                        axis=0,
                    )
                    y = y + lax.dot_general(
                        tap_rows(w_ref, a, channels), window, NT, preferred_element_type=jnp.float32
                    )
                out = column_shift(y, shard, width) + t_ref[:, :1]
                eo_ref[:, q * edge : (q + 1) * edge] = out[:, :edge].astype(jnp.bfloat16)
                mo_ref[:, q * mid : (q + 1) * mid] = out[:, edge:].astype(jnp.bfloat16)
                fe_ref[:, q * edge : (q + 1) * edge] = lax.dot_general(
                    p_ref[...], e, NT, preferred_element_type=jnp.float32
                ).astype(jnp.bfloat16)
                fm_ref[:, q * mid : (q + 1) * mid] = lax.dot_general(
                    p_ref[...], m, NT, preferred_element_type=jnp.float32
                ).astype(jnp.bfloat16)
                out_buf[q] = out
                sums = jnp.where(lane == q, jnp.sum(out, axis=1, keepdims=True), sums)
        centers = jnp.dot(g_ref[...], sums, precision=HIGHEST) / (length * group)
        sums = jnp.zeros((shard, LANES), jnp.float32)
        for q in range(count):
            c = out_buf[q] - centers[:, q : q + 1]
            sums = jnp.where(lane == q, jnp.sum(c * c, axis=1, keepdims=True), sums)
        squares = jnp.dot(g_ref[...], sums, precision=HIGHEST)
        for start, found in ((0, centers), (count, squares)):
            so_ref[start : start + count] = lax.dot_general(
                i_ref[...], found, NT, precision=HIGHEST
            )[:count]

    out_shape = (
        jax.ShapeDtypeStruct((shard, count * edge), jnp.bfloat16),
        jax.ShapeDtypeStruct((shard, count * mid), jnp.bfloat16),
        jax.ShapeDtypeStruct((2 * count, shard), jnp.float32),
        jax.ShapeDtypeStruct((shard, count * edge), jnp.bfloat16),
        jax.ShapeDtypeStruct((shard, count * mid), jnp.bfloat16),
    )
    scratch = [
        pltpu.VMEM((length + 2 * width, channels), jnp.bfloat16),
        pltpu.VMEM((count, shard, length), jnp.float32),
    ]
    return call(body, out_shape, scratch, scalars=1, flops=6 * count * length * channels * 3 * shard)(
        ends, *edges, *mids, above, below, weight, bias, groups, pick, eye
    )


def second_conv(ends, edges, mids, above, below, weight, own_edges, own_mids, samples, width):
    n = len(edges)
    shard = edges[0].shape[0]
    count = n * samples
    edge, mid = edges[0].shape[1] // count, (mids[0].shape[1] - LANES) // count
    length = edge + mid

    unrolled = n <= 4
    shape = jax.ShapeDtypeStruct((samples, shard, length), jnp.bfloat16)
    if not unrolled:
        shape = jax.ShapeDtypeStruct((n, samples, shard, length), jnp.bfloat16)

    def body(*refs):
        ends_ref = refs[0]
        e_refs, m_refs = refs[1 : 1 + n], refs[1 + n : 1 + 2 * n]
        a_ref, b_ref, w_ref, fe_ref, fm_ref = refs[1 + 2 * n : 6 + 2 * n]
        o_refs, buf = refs[6 + 2 * n : -1], refs[-1]
        low = lax.broadcasted_iota(jnp.int32, (shard, edge), 1) < width
        inside = jnp.where(low, ends_ref[0], ends_ref[1]).astype(jnp.float32)

        def sample(t, i, slot):
            for j in range(n):
                q = ((t - j) % n if unrolled else lax.rem(t - j + n, n)) * samples + i
                tail = m_refs[j][:, count * mid :]
                mean = spread_column(tail, q, 2 * count)
                scale = spread_column(tail, q + count, 2 * count)

                def act(x):
                    return silu((x - mean) * scale)

                rows = slice(j * shard, (j + 1) * shard)
                natural = pl.ds(pl.multiple_of(lax.rem(ends_ref[2] + n - j, n) * shard, 16), shard)
                half = q // 2 if unrolled else lax.div(q, 2)
                last = a_ref[rows, tile(half, edge)].astype(jnp.float32)
                first = b_ref[rows, tile(half, edge)].astype(jnp.float32)
                if unrolled:
                    odd = q % 2 == 1
                    halo = (
                        jnp.where(low, pltpu.roll(last, width, axis=1), first)
                        if odd
                        else jnp.where(low, last, pltpu.roll(first, width, axis=1))
                    )
                else:
                    halo = jnp.where(
                        lax.rem(q, 2) == 1,
                        jnp.where(low, pltpu.roll(last, width, axis=1), first),
                        jnp.where(low, last, pltpu.roll(first, width, axis=1)),
                    )
                halo = (act(halo) * inside).astype(jnp.bfloat16)
                e = act(e_refs[j][:, tile(q, edge)].astype(jnp.float32))
                m = act(m_refs[j][:, tile(q, mid)].astype(jnp.float32))
                turned = pltpu.roll(m, width, axis=1).astype(jnp.bfloat16)
                e = e.astype(jnp.bfloat16)
                m = m.astype(jnp.bfloat16)
                buf[slot, 0, natural, :edge] = jnp.where(low, halo, m)
                buf[slot, 0, natural, edge:] = jnp.where(low, e, turned)
                buf[slot, 1, natural, :edge] = e
                buf[slot, 1, natural, edge:] = m
                buf[slot, 2, natural, :edge] = jnp.where(low, m, halo)
                buf[slot, 2, natural, edge:] = jnp.where(low, turned, e)
            y = jnp.zeros((3 * shard, length), jnp.float32)
            for a in range(3):
                y = y + jnp.dot(
                    tap_rows(w_ref, a, n * shard), buf[slot, a], preferred_element_type=jnp.float32
                )
            out = column_shift(y, shard, width)
            q = t * samples + i
            target = o_refs[t].at[i] if unrolled else o_refs[0].at[t, i]
            target[:, :edge] = (
                out[:, :edge] + fe_ref[:, tile(q, edge)].astype(jnp.float32)
            ).astype(jnp.bfloat16)
            target[:, edge:] = (
                out[:, edge:] + fm_ref[:, tile(q, mid)].astype(jnp.float32)
            ).astype(jnp.bfloat16)

        if unrolled:
            for q in range(count):
                sample(q // samples, q % samples, q % 2)
        else:

            @pl.loop(0, n)
            def _(t):
                for i in range(samples):
                    sample(t, i, 0)

    result = call(
        body,
        (shape,) * n if unrolled else shape,
        [pltpu.VMEM((2 if unrolled else 1, 3, n * shard, length), jnp.bfloat16)],
        scalars=1,
        flops=6 * count * length * n * shard * 3 * shard,
    )(ends, *edges, *mids, above, below, weight, own_edges, own_mids)
    return result if unrolled else [result[t] for t in range(n)]


def split_dot(ones, column):
    high = column.astype(jnp.bfloat16)
    rest = column - high.astype(jnp.float32)
    middle = rest.astype(jnp.bfloat16)
    low = (rest - middle.astype(jnp.float32)).astype(jnp.bfloat16)
    lane = lax.broadcasted_iota(jnp.int32, (column.shape[0], LANES), 1)
    parts = jnp.where(lane == 0, high.astype(jnp.float32), 0.0)
    parts = jnp.where(lane == 1, middle.astype(jnp.float32), parts)
    parts = jnp.where(lane == 2, low.astype(jnp.float32), parts).astype(jnp.bfloat16)
    summed = jnp.dot(ones, parts, preferred_element_type=jnp.float32)
    return jnp.sum(summed, axis=1, keepdims=True)


def attention(where, chunks, weights, gain, spread, unpad, wide, width, group):
    pieces, parts = len(chunks), len(weights)
    samples, rows, length = chunks[0].shape
    channels = rows if unpad is None else unpad.shape[1]
    heads = channels // HEAD_DIM
    keys = pieces * length
    inner = length // width - 2
    packed = parts > 1

    def body(*refs):
        where_ref, c_refs = refs[0], refs[1 : 1 + pieces]
        w_refs = refs[1 + pieces : 1 + pieces + parts]
        g_ref, a_ref, b_ref = refs[1 + pieces + parts : 4 + pieces + parts]
        o_ref, buf, query_buf, mixed_buf = refs[-4 - packed : len(refs) - packed]
        weight = refs[-1] if packed else w_refs[0]
        if packed:
            blocks, part, _ = weights[0].shape
            steps = wide // part
            for k, w in enumerate(w_refs):
                at = where_ref[k]
                for g in range(blocks):
                    start = jnp.where(
                        at < steps,
                        g * wide + at * part,
                        blocks * wide + g * (channels // blocks) + (at - steps) * part,
                    )
                    weight[pl.ds(pl.multiple_of(start, 16), part)] = w[g]
        for i in range(samples):
            total = jnp.zeros((rows, LANES), jnp.float32)
            for c in c_refs:
                for start in range(0, length, LANES):
                    total = total + c[i, :, start : start + LANES].astype(jnp.float32)
            total = jnp.sum(total, axis=1, keepdims=True)
            mean = split_dot(b_ref[...], split_dot(a_ref[...], total)) / (keys * group)
            total = jnp.zeros((rows, LANES), jnp.float32)
            for c in c_refs:
                for start in range(0, length, LANES):
                    away = c[i, :, start : start + LANES].astype(jnp.float32) - mean
                    total = total + away * away
            total = jnp.sum(total, axis=1, keepdims=True)
            spread_of = split_dot(b_ref[...], split_dot(a_ref[...], total)) / (keys * group)
            scale = lax.rsqrt(spread_of + EPSILON) * g_ref[:, :1]
            for p, c in enumerate(c_refs):
                normed = ((c[i].astype(jnp.float32) - mean) * scale).astype(jnp.bfloat16)
                if p == 0:
                    queries = jnp.dot(
                        weight[:channels, :rows], normed, preferred_element_type=jnp.float32
                    )
                    queries = queries.astype(jnp.bfloat16).astype(jnp.float32) * HEAD_DIM ** (-0.5)
                    query_buf[...] = queries.T.astype(jnp.bfloat16)
                buf[:, p * length : (p + 1) * length] = jnp.dot(
                    weight[channels : 3 * channels, :rows],
                    normed,
                    preferred_element_type=jnp.float32,
                ).astype(jnp.bfloat16)

            @pl.loop(0, heads // 2)
            def _(two):
                lanes = pl.ds(pl.multiple_of(two * LANES, LANES), LANES)
                k_two = buf[pl.ds(pl.multiple_of(two * LANES, LANES), LANES)]
                v_two = buf[pl.ds(pl.multiple_of(channels + two * LANES, LANES), LANES)]
                q_two = query_buf[:, lanes]
                pair = []
                for h in range(2):
                    cut = slice(h * HEAD_DIM, (h + 1) * HEAD_DIM)
                    scores = jnp.dot(q_two[:, cut], k_two[cut], preferred_element_type=jnp.float32)
                    shifted = jnp.exp(scores - jnp.max(scores, axis=1, keepdims=True))
                    totals = jnp.sum(shifted, axis=1, keepdims=True)
                    mixed = lax.dot_general(
                        shifted.astype(jnp.bfloat16),
                        v_two[cut],
                        NT,
                        preferred_element_type=jnp.float32,
                    )
                    pair.append(mixed / totals)
                mixed_buf[:, lanes] = jnp.concatenate(pair, axis=1).astype(jnp.bfloat16)

            own = c_refs[0][i].astype(jnp.float32).T
            if unpad is not None:
                own = jnp.dot(
                    own.astype(jnp.bfloat16),
                    refs[4 + pieces + parts][...],
                    preferred_element_type=jnp.float32,
                )
            result = own + lax.dot_general(
                mixed_buf[...],
                weight[3 * channels :, :channels],
                NT,
                preferred_element_type=jnp.float32,
            )
            result = result.astype(jnp.bfloat16)
            o_ref[i, 0] = result[:width]
            o_ref[i, 1 + inner] = result[width : 2 * width]
            for r in range(inner):
                o_ref[i, 1 + r] = result[(2 + r) * width : (3 + r) * width]

    operands = [*chunks, *weights, gain, spread.T, spread]
    if unpad is not None:
        operands.append(unpad)
    scratch = [
        pltpu.VMEM((2 * channels, keys), jnp.bfloat16),
        pltpu.VMEM((length, channels), jnp.bfloat16),
        pltpu.VMEM((length, channels), jnp.bfloat16),
    ]
    if packed:
        scratch.append(pltpu.VMEM((4 * channels, rows), jnp.bfloat16))
    return call(
        body,
        jax.ShapeDtypeStruct((samples, length // width, width, channels), jnp.bfloat16),
        scratch,
        scalars=1,
    )(where, *operands)


def pad_rows(values, rows, axis):
    missing = rows - values.shape[axis]
    return jnp.pad(values, [(0, missing if a == axis else 0) for a in range(values.ndim)])


def local(
    features,
    step_index,
    roster,
    time_weight,
    temb_weight,
    norm_gains,
    conv_first,
    conv_second,
    attn_weight,
    out_weight,
):
    samples, height, width, channels = features.shape
    n, planes = lax.axis_size("fsdp"), lax.axis_size("spatial")
    mine, row = lax.axis_index("fsdp"), lax.axis_index("spatial")
    group = channels // GROUPS
    kept = conv_first.shape[1]
    shard = -(-kept // 16) * 16
    length = height * width
    entries = float(length * group)
    count = n * samples
    half = planes // 2
    swap = [(i, i ^ 1) for i in range(planes)]
    ends = jnp.stack([row > 0, row < planes - 1, mine]).astype(jnp.int32)

    def ring(values):
        return [values] + [shift(values, "fsdp", j) for j in range(1, n)]

    def block(values, axis):
        return lax.dynamic_slice_in_dim(values, mine * kept, kept, axis)

    def pad_blocks(values, axis):
        if shard == kept:
            return values
        shape = list(values.shape)
        parts = values.reshape(shape[:axis] + [shape[axis] // kept, kept] + shape[axis + 1 :])
        parts = pad_rows(parts, shard, axis + 1)
        return parts.reshape(shape[:axis] + [shape[axis] // kept * shard] + shape[axis + 1 :])

    def in_plane_stats(values):
        values = values[None]
        size = 1
        while size < planes:
            other = lax.ppermute(values, "spatial", [(i, i ^ size) for i in range(planes)])
            values = jnp.concatenate([values, other], axis=0)
            size *= 2
        return values

    def in_plane(values):
        near = [values] + [shift(values, "spatial", 2 * d) for d in range(1, half)]
        far = [lax.ppermute(c, "spatial", swap) for c in near]
        back = (row - 2 * np.arange(half)) % planes
        return near + far, jnp.concatenate([back, back ^ 1]).astype(jnp.int32)

    flat = features.reshape(samples, length, channels)
    own_stats = local_stats(flat, members(channels, channels, channels, group), group)
    edges = ring(jnp.concatenate([flat[:, :width], flat[:, length - width :]], axis=1))
    last, first = halo_rows(edges, width)
    above = shift_rows(last, 1)
    below = shift_rows(first, -1)
    own_stats = in_plane_stats(own_stats)
    mids = rows_message(own_stats, norm_gains[:1], entries, flat[:, width : length - width])
    mids = ring(mids)

    wide = attn_weight.shape[1]
    part = -(-(wide + kept) // (16 * planes)) * 16
    turned = jnp.concatenate(
        [pad_blocks(attn_weight.T, 1), pad_rows(out_weight.T, n * shard, 1)], axis=0
    )
    turned = lax.dynamic_slice_in_dim(pad_rows(turned, part * planes, 0), row * part, part, 0)
    places = ((mine - np.arange(n)) % n).astype(jnp.int32)
    pieces = ring(turned[None])
    turned = place(places, pieces, 0)
    projection, from_rows = in_plane(turned)
    if wide % part or kept % part:
        turned = place(from_rows, projection, 1)
        projection = [
            jnp.concatenate(
                [
                    turned[:, :wide].reshape(n * wide, n * shard),
                    turned[:, wide : wide + kept].reshape(channels, n * shard),
                ]
            )
        ]

    first_weight = pad_rows(conv_first.T, shard, 0)
    second_weight = pad_rows(pad_blocks(conv_second.T, 1), shard, 0)
    bias = time_bias(step_index, roster, time_weight, block(temb_weight, 1), shard)
    index = jnp.arange(shard)
    pick = jnp.where(index < kept, index + mine * kept, -1)[:, None] == jnp.arange(channels)[None, :]

    edges, mids, own_stats, own_edges, own_mids = first_conv(
        ends,
        edges,
        mids,
        above,
        below,
        first_weight,
        bias,
        same_group(shard, shard, kept, group),
        pick.astype(jnp.bfloat16),
        jnp.asarray(np.eye(-(-count // 8) * 8, LANES, dtype=np.float32)),
        width,
        group,
    )

    edges = ring(edges)
    last, first = halo_columns(edges, width)
    above = shift_rows(last, 1)
    below = shift_rows(first, -1)
    gain = pad_rows(block(norm_gains[1:2], 1), shard, 1)
    own_stats = in_plane_stats(own_stats)
    mids = columns_message(own_stats, gain, entries, mids)
    mids = ring(mids)
    sums = second_conv(
        ends,
        edges,
        mids,
        above,
        below,
        second_weight,
        own_edges,
        own_mids,
        samples,
        width,
    )

    own = [sums[0]] + [shift(sums[t], "fsdp", -t) for t in range(1, n)]
    own = place(((mine + np.arange(n)) % n).astype(jnp.int32), own, 1)
    chunks, _ = in_plane(own)
    gain = jnp.broadcast_to(pad_blocks(norm_gains[2], 0)[:, None], (n * shard, LANES))
    unpad = None
    if shard != kept:
        at = np.arange(n * shard)
        at = np.where(at % shard < kept, at // shard * kept + at % shard, -1)
        unpad = jnp.asarray(at[:, None] == np.arange(channels)[None, :], jnp.bfloat16)
    return attention(
        from_rows,
        chunks,
        projection,
        gain,
        members(n * shard, shard, kept, group),
        unpad,
        wide,
        width,
        group,
    )


def shift_rows(values, step):
    count = lax.axis_size("spatial")
    pairs = [(i, i + step) for i in range(count) if 0 <= i + step < count]
    return lax.ppermute(values, "spatial", pairs)


def solution(mesh):
    in_specs = (
        P("fsdp", "spatial", None, None),
        P(),
        P(),
        P(),
        P(),
        P(),
        P(None, "fsdp"),
        P(None, "fsdp"),
        P(None, "fsdp"),
        P(None, "fsdp"),
    )
    out_specs = P("fsdp", "spatial", None, None)

    return jax.shard_map(local, mesh=mesh, in_specs=in_specs, out_specs=out_specs, check_vma=False)
```

```python
import math

import jax
import jax.numpy as jnp
import numpy as np
from jax import lax
from jax.experimental import pallas as pl
from jax.experimental.pallas import tpu as pltpu
from jax.sharding import PartitionSpec as P


HEAD_DIM = 64
GROUPS = 32
EPSILON = 1e-05
LANES = 128
HIGHEST = lax.Precision.HIGHEST


NT = (((1,), (1,)), ((), ()))


def call(body, out_shape, scratch=(), scalars=0, flops=0):
    def run(*operands):
        specs = [
            pl.BlockSpec(memory_space=pltpu.SMEM if i < scalars else pltpu.VMEM)
            for i in range(len(operands))
        ]
        outs = jax.tree.map(lambda _: pl.BlockSpec(memory_space=pltpu.VMEM), out_shape)
        return pl.pallas_call(
            body,
            out_shape=out_shape,
            in_specs=specs,
            out_specs=outs,
            scratch_shapes=list(scratch),
            compiler_params=pltpu.CompilerParams(vmem_limit_bytes=60 * 2**20),
            cost_estimate=pl.CostEstimate(flops=flops, transcendentals=0, bytes_accessed=0)
            if flops
            else None,
        )(*operands)

    return run


def shift(values, axis, step):
    count = lax.axis_size(axis)
    return lax.ppermute(values, axis, [(i, (i + step) % count) for i in range(count)])


def silu(v):
    half = 0.5 * v
    return half + half * jnp.tanh(half)


def own_channels(where, rows, kept, channels):
    row = lax.broadcasted_iota(jnp.int32, (rows, channels), 0)
    column = lax.broadcasted_iota(jnp.int32, (rows, channels), 1)
    chosen = (row + where * kept == column) & (row < kept)
    return jnp.where(chosen, 1.0, 0.0).astype(jnp.bfloat16)


def part_rows(row):
    at = lax.broadcasted_iota(jnp.int32, (8, row.shape[1]), 0)
    high, middle, low = three_parts(row)
    parts = jnp.where(at == 0, high, jnp.where(at == 1, middle, jnp.where(at == 2, low, 0.0)))
    return parts.astype(jnp.bfloat16)


def time_bias(ends, step_index, roster, time_weight, temb_weight, rows, kept):
    freqs, hidden = time_weight.shape
    channels = temb_weight.shape[1]
    half_len = freqs // 2
    steps = roster.shape[0]

    def column(row):
        tiles = [
            jnp.broadcast_to(row[:, start : start + LANES], (LANES, LANES)).T
            for start in range(0, row.shape[1], LANES)
        ]
        return jnp.concatenate(tiles, axis=0)[:, :1]

    def body(n_ref, i_ref, r_ref, w_ref, t_ref, o_ref):
        at = lax.broadcasted_iota(jnp.int32, (1, steps), 1)
        moment = jnp.sum(jnp.where(at == i_ref[0], r_ref[...], 0.0), axis=1, keepdims=True)
        padded = -(-half_len // LANES) * LANES
        place = lax.broadcasted_iota(jnp.int32, (1, padded), 1).astype(jnp.float32)
        angles = moment * jnp.exp(-math.log(10000.0) * place / half_len)
        time_hidden = jnp.zeros((1, hidden), jnp.float32)
        for start, wave in ((0, jnp.cos(angles)), (half_len, jnp.sin(angles))):
            time_hidden = time_hidden + jnp.sum(
                column(wave)[:half_len] * w_ref[start : start + half_len], axis=0, keepdims=True
            )
        time_hidden = time_hidden / (1.0 + jnp.exp(-time_hidden))
        summed = jnp.zeros((LANES, channels), jnp.float32)
        turned = column(time_hidden)
        for start in range(0, hidden, LANES):
            summed = summed + turned[start : start + LANES] * t_ref[start : start + LANES]
        parts = lax.dot_general(
            own_channels(n_ref[2], rows, kept, channels),
            part_rows(jnp.sum(summed, axis=0, keepdims=True)),
            NT,
            preferred_element_type=jnp.float32,
        )
        o_ref[...] = jnp.broadcast_to(jnp.sum(parts, axis=1, keepdims=True), (rows, LANES))

    return call(body, jax.ShapeDtypeStruct((rows, LANES), jnp.float32), scalars=2)(
        ends, step_index, roster[None, :], time_weight, temb_weight
    )


def group_of(rows, block, kept, width):
    index = np.arange(rows)
    group = (index // block * kept + index % block) // width
    return np.where(index % block < kept, group, -1)


def members(rows, block, kept, width):
    group = group_of(rows, block, kept, width)[:, None]
    return jnp.asarray(group == np.arange(LANES)[None, :], jnp.bfloat16)


def same_group(rows, block, kept, width):
    group = group_of(rows, block, kept, width)[:, None]
    return jnp.asarray((group == group.T) & (group >= 0), jnp.float32)


def three_parts(values):
    high = values.astype(jnp.bfloat16).astype(jnp.float32)
    rest = values - high
    middle = rest.astype(jnp.bfloat16).astype(jnp.float32)
    return high, middle, rest - middle


def group_sums(row, member):
    for dims in ((((1,), (0,)), ((), ())), NT):
        summed = lax.dot_general(
            part_rows(row), member, dims, preferred_element_type=jnp.float32
        )
        row = jnp.sum(summed, axis=0, keepdims=True)
    return row


def local_stats(features, member, width, columns):
    samples, length, channels = features.shape

    def body(x_ref, g_ref, o_ref, e_ref):
        for i in range(samples):
            e_ref[i, :columns] = x_ref[i, :columns]
            e_ref[i, columns:] = x_ref[i, length - columns :]
            v = x_ref[i].astype(jnp.float32)
            mean = group_sums(jnp.sum(v, axis=0, keepdims=True), g_ref[...]) / (length * width)
            c = v - mean
            o_ref[i : i + 1] = mean
            o_ref[samples + i : samples + i + 1] = group_sums(
                jnp.sum(c * c, axis=0, keepdims=True), g_ref[...]
            )

    shapes = (
        jax.ShapeDtypeStruct((2 * samples, channels), jnp.float32),
        jax.ShapeDtypeStruct((samples, 2 * columns, channels), jnp.bfloat16),
    )
    return call(body, shapes)(features, member)


def place_weights(where, pieces, wide, channels):
    blocks, part, depth = pieces[0].shape
    steps = wide // part

    def body(w_ref, *refs):
        for k, piece in enumerate(refs[:-1]):
            at = w_ref[k]
            for g in range(blocks):
                start = jnp.where(
                    at < steps,
                    g * wide + at * part,
                    blocks * wide + g * (channels // blocks) + (at - steps) * part,
                )
                refs[-1][pl.ds(pl.multiple_of(start, 16), part)] = piece[g]

    shape = jax.ShapeDtypeStruct((4 * channels, depth), jnp.bfloat16)
    return call(body, shape, scalars=1)(where, *pieces)


def place(where, pieces, axis, flops=0):
    first = pieces[0]
    size = first.shape[axis]
    shape = list(first.shape)
    shape[axis] = size * len(pieces)

    def body(w_ref, *refs):
        for k, piece in enumerate(refs[:-1]):
            start = pl.multiple_of(w_ref[k] * size, size)
            refs[-1][(slice(None),) * axis + (pl.ds(start, size),)] = piece[...]

    return call(body, jax.ShapeDtypeStruct(tuple(shape), first.dtype), scalars=1, flops=flops)(
        where, *pieces
    )


def norm_terms(figures, gain, entries):
    count = figures.shape[0] // 2
    return figures[:count], lax.rsqrt(figures[count:] / entries + EPSILON) * gain


TAIL = 16


def rows_message(figures, gain, entries, flat, width):
    samples, length, channels = flat.shape
    mid = length - 2 * width

    def body(p_ref, g_ref, m_ref, o_ref):
        mean, scale = norm_terms(p_ref[...], g_ref[...], entries)
        for i in range(samples):
            o_ref[i, :mid] = m_ref[i, width : width + mid]
            rows = [*three_parts(mean[i : i + 1]), *three_parts(scale[i : i + 1])]
            rows.append(jnp.zeros((TAIL - len(rows), channels), jnp.float32))
            o_ref[i, mid:] = jnp.concatenate(rows, axis=0).astype(jnp.bfloat16)

    shape = jax.ShapeDtypeStruct((samples, mid + TAIL, channels), jnp.bfloat16)
    return call(body, shape)(figures, gain, flat)


def columns_message(figures, gain, entries, mids):
    shard, wide = mids.shape

    def body(p_ref, g_ref, m_ref, o_ref):
        o_ref[:, :wide] = m_ref[...]
        terms = jnp.concatenate(norm_terms(p_ref[...], g_ref[...], entries), axis=0)
        rows = [*three_parts(terms)]
        rows.append(jnp.zeros((LANES - 3 * terms.shape[0], shard), jnp.float32))
        rows = jnp.concatenate(rows, axis=0).astype(jnp.bfloat16)
        o_ref[:, wide:] = lax.dot_general(
            identity(shard, shard), rows, NT, preferred_element_type=jnp.float32
        ).astype(jnp.bfloat16)

    shape = jax.ShapeDtypeStruct((shard, wide + LANES), jnp.bfloat16)
    return call(body, shape)(figures, gain, mids)


def identity(rows, columns):
    at = lax.broadcasted_iota(jnp.int32, (rows, columns), 0)
    same = at == lax.broadcasted_iota(jnp.int32, (rows, columns), 1)
    return jnp.where(same, 1.0, 0.0).astype(jnp.bfloat16)


def halo_rows(edges, width):
    samples, _, channels = edges[0].shape
    shape = jax.ShapeDtypeStruct((len(edges) * samples, width, channels), jnp.bfloat16)

    def body(*refs):
        for j, e in enumerate(refs[:-2]):
            refs[-2][j * samples : (j + 1) * samples] = e[:, width:]
            refs[-1][j * samples : (j + 1) * samples] = e[:, :width]

    return call(body, (shape, shape))(*edges)


def halo_columns(edges, width):
    shard, wide = edges[0].shape
    edge = 2 * width
    shape = jax.ShapeDtypeStruct((len(edges) * shard, wide // 2), jnp.bfloat16)

    def body(*refs):
        low = lax.broadcasted_iota(jnp.int32, (shard, edge), 1) < width
        for j, e in enumerate(refs[:-2]):
            rows = slice(j * shard, (j + 1) * shard)
            for p in range(wide // edge // 2):
                left = e[:, 2 * p * edge : (2 * p + 1) * edge].astype(jnp.float32)
                right = e[:, (2 * p + 1) * edge : (2 * p + 2) * edge].astype(jnp.float32)
                cut = slice(p * edge, (p + 1) * edge)
                last = jnp.where(low, pltpu.roll(left, width, axis=1), right)
                first = jnp.where(low, left, pltpu.roll(right, width, axis=1))
                refs[-2][rows, cut] = last.astype(jnp.bfloat16)
                refs[-1][rows, cut] = first.astype(jnp.bfloat16)

    return call(body, (shape, shape))(*edges)


def tap_rows(weight, row, depth):
    return jnp.concatenate(
        [weight[:, (3 * row + b) * depth : (3 * row + b + 1) * depth] for b in range(3)], axis=0
    )


def spread_column(tail, at, period):
    lane = lax.broadcasted_iota(jnp.int32, (LANES, LANES), 0)
    chosen = (lane == at) | (lane == at + period) | (lane == at + 2 * period)
    chosen = jnp.where(chosen, 1.0, 0.0).astype(jnp.bfloat16)
    return jnp.dot(tail, chosen, preferred_element_type=jnp.float32)


def tile(index, size):
    if isinstance(index, int):
        return slice(index * size, (index + 1) * size)
    return pl.ds(pl.multiple_of(index * size, LANES), size)


def column_shift(y, shard, width):
    lane = lax.broadcasted_iota(jnp.int32, (shard, LANES), 1) % width
    tiles = []
    for start in range(0, y.shape[1], LANES):
        left = y[:shard, start : start + LANES]
        right = y[2 * shard :, start : start + LANES]
        tiles.append(
            y[shard : 2 * shard, start : start + LANES]
            + jnp.where(lane > 0, pltpu.roll(left, 1, axis=1), 0.0)
            + jnp.where(lane < width - 1, pltpu.roll(right, LANES - 1, axis=1), 0.0)
        )
    return jnp.concatenate(tiles, axis=1)


def first_conv(ends, edges, mids, above, below, weight, bias, groups, gain, eye, kept, width, group):
    n = len(edges)
    samples, edge, channels = edges[0].shape
    mid = mids[0].shape[1] - TAIL
    shard = bias.shape[0]
    count = n * samples
    inner = mid // width
    length = edge + mid

    def body(*refs):
        ends_ref = refs[0]
        e_refs, m_refs = refs[1 : 1 + n], refs[1 + n : 1 + 2 * n]
        a_ref, b_ref, w_ref, t_ref, g_ref, p_ref, i_ref = refs[1 + 2 * n : 8 + 2 * n]
        eo_ref, mo_ref, so_ref, fe_ref, fm_ref, go_ref, buf, out_buf = refs[8 + 2 * n :]
        pick = own_channels(ends_ref[2], shard, kept, channels)
        parts = lax.dot_general(part_rows(p_ref[...]), pick, NT, preferred_element_type=jnp.float32)
        go_ref[...] = jnp.sum(parts, axis=0, keepdims=True)
        has_above = ends_ref[0].astype(jnp.float32)
        has_below = ends_ref[1].astype(jnp.float32)
        lane = lax.broadcasted_iota(jnp.int32, (shard, LANES), 1)
        sums = jnp.zeros((shard, LANES), jnp.float32)
        for j in range(n):
            for i in range(samples):
                q = j * samples + i
                tail = m_refs[j][i, mid:].astype(jnp.float32)
                mean = tail[0:1] + tail[1:2] + tail[2:3]
                scale = tail[3:4] + tail[4:5] + tail[5:6]

                def act(x):
                    return silu((x.astype(jnp.float32) - mean) * scale)

                e = e_refs[j][i]
                m = m_refs[j][i, :mid]
                ea = act(e).astype(jnp.bfloat16)
                buf[q % 2, :width] = (act(a_ref[q]) * has_above).astype(jnp.bfloat16)
                buf[q % 2, width : 2 * width] = ea[:width]
                buf[q % 2, 2 * width : 2 * width + mid] = act(m).astype(jnp.bfloat16)
                buf[q % 2, 2 * width + mid : 3 * width + mid] = ea[width:]
                buf[q % 2, 3 * width + mid :] = (act(b_ref[q]) * has_below).astype(jnp.bfloat16)
                y = jnp.zeros((3 * shard, length), jnp.float32)
                for a in range(3):
                    window = jnp.concatenate(
                        [
                            buf[q % 2, a * width : (a + 1) * width],
                            buf[q % 2, (a + 1 + inner) * width : (a + 2 + inner) * width],
                            buf[q % 2, (a + 1) * width : (a + 1 + inner) * width],
                        ],
                        axis=0,
                    )
                    y = y + lax.dot_general(
                        tap_rows(w_ref, a, channels), window, NT, preferred_element_type=jnp.float32
                    )
                out = column_shift(y, shard, width) + t_ref[:, :1]
                eo_ref[:, q * edge : (q + 1) * edge] = out[:, :edge].astype(jnp.bfloat16)
                mo_ref[:, q * mid : (q + 1) * mid] = out[:, edge:].astype(jnp.bfloat16)
                fe_ref[:, q * edge : (q + 1) * edge] = lax.dot_general(
                    pick, e, NT, preferred_element_type=jnp.float32
                ).astype(jnp.bfloat16)
                fm_ref[:, q * mid : (q + 1) * mid] = lax.dot_general(
                    pick, m, NT, preferred_element_type=jnp.float32
                ).astype(jnp.bfloat16)
                out_buf[q] = out
                sums = jnp.where(lane == q, jnp.sum(out, axis=1, keepdims=True), sums)
        centers = jnp.dot(g_ref[...], sums, precision=HIGHEST) / (length * group)
        sums = jnp.zeros((shard, LANES), jnp.float32)
        for q in range(count):
            c = out_buf[q] - centers[:, q : q + 1]
            sums = jnp.where(lane == q, jnp.sum(c * c, axis=1, keepdims=True), sums)
        squares = jnp.dot(g_ref[...], sums, precision=HIGHEST)
        for start, found in ((0, centers), (count, squares)):
            so_ref[start : start + count] = lax.dot_general(
                i_ref[...], found, NT, precision=HIGHEST
            )[:count]

    out_shape = (
        jax.ShapeDtypeStruct((shard, count * edge), jnp.bfloat16),
        jax.ShapeDtypeStruct((shard, count * mid), jnp.bfloat16),
        jax.ShapeDtypeStruct((2 * count, shard), jnp.float32),
        jax.ShapeDtypeStruct((shard, count * edge), jnp.bfloat16),
        jax.ShapeDtypeStruct((shard, count * mid), jnp.bfloat16),
        jax.ShapeDtypeStruct((1, shard), jnp.float32),
    )
    scratch = [
        pltpu.VMEM((2, length + 2 * width, channels), jnp.bfloat16),
        pltpu.VMEM((count, shard, length), jnp.float32),
    ]
    return call(body, out_shape, scratch, scalars=1, flops=6 * count * length * channels * 3 * shard)(
        ends, *edges, *mids, above, below, weight, bias, groups, gain, eye
    )


def second_conv(ends, edges, mids, above, below, weight, own_edges, own_mids, samples, width):
    n = len(edges)
    shard = edges[0].shape[0]
    count = n * samples
    edge, mid = edges[0].shape[1] // count, (mids[0].shape[1] - LANES) // count
    length = edge + mid

    unrolled = n <= 4
    shape = jax.ShapeDtypeStruct((samples, shard, length), jnp.bfloat16)
    if not unrolled:
        shape = jax.ShapeDtypeStruct((n, samples, shard, length), jnp.bfloat16)

    def body(*refs):
        ends_ref = refs[0]
        e_refs, m_refs = refs[1 : 1 + n], refs[1 + n : 1 + 2 * n]
        a_ref, b_ref, w_ref, fe_ref, fm_ref = refs[1 + 2 * n : 6 + 2 * n]
        o_refs, buf = refs[6 + 2 * n : -1], refs[-1]
        low = lax.broadcasted_iota(jnp.int32, (shard, edge), 1) < width
        inside = jnp.where(low, ends_ref[0], ends_ref[1]).astype(jnp.float32)

        def sample(t, i, slot):
            for j in range(n):
                q = ((t - j) % n if unrolled else lax.rem(t - j + n, n)) * samples + i
                tail = m_refs[j][:, count * mid :]
                mean = spread_column(tail, q, 2 * count)
                scale = spread_column(tail, q + count, 2 * count)

                def act(x):
                    return silu((x - mean) * scale)

                rows = slice(j * shard, (j + 1) * shard)
                natural = pl.ds(pl.multiple_of(lax.rem(ends_ref[2] + n - j, n) * shard, 16), shard)
                half = q // 2 if unrolled else lax.div(q, 2)
                last = a_ref[rows, tile(half, edge)].astype(jnp.float32)
                first = b_ref[rows, tile(half, edge)].astype(jnp.float32)
                if unrolled:
                    odd = q % 2 == 1
                    halo = (
                        jnp.where(low, pltpu.roll(last, width, axis=1), first)
                        if odd
                        else jnp.where(low, last, pltpu.roll(first, width, axis=1))
                    )
                else:
                    halo = jnp.where(
                        lax.rem(q, 2) == 1,
                        jnp.where(low, pltpu.roll(last, width, axis=1), first),
                        jnp.where(low, last, pltpu.roll(first, width, axis=1)),
                    )
                halo = (act(halo) * inside).astype(jnp.bfloat16)
                e = act(e_refs[j][:, tile(q, edge)].astype(jnp.float32))
                m = act(m_refs[j][:, tile(q, mid)].astype(jnp.float32))
                turned = pltpu.roll(m, width, axis=1).astype(jnp.bfloat16)
                e = e.astype(jnp.bfloat16)
                m = m.astype(jnp.bfloat16)
                buf[slot, 0, natural, :edge] = jnp.where(low, halo, m)
                buf[slot, 0, natural, edge:] = jnp.where(low, e, turned)
                buf[slot, 1, natural, :edge] = e
                buf[slot, 1, natural, edge:] = m
                buf[slot, 2, natural, :edge] = jnp.where(low, m, halo)
                buf[slot, 2, natural, edge:] = jnp.where(low, turned, e)
            y = jnp.zeros((3 * shard, length), jnp.float32)
            for a in range(3):
                y = y + jnp.dot(
                    tap_rows(w_ref, a, n * shard), buf[slot, a], preferred_element_type=jnp.float32
                )
            out = column_shift(y, shard, width)
            q = t * samples + i
            target = o_refs[t].at[i] if unrolled else o_refs[0].at[t, i]
            target[:, :edge] = (
                out[:, :edge] + fe_ref[:, tile(q, edge)].astype(jnp.float32)
            ).astype(jnp.bfloat16)
            target[:, edge:] = (
                out[:, edge:] + fm_ref[:, tile(q, mid)].astype(jnp.float32)
            ).astype(jnp.bfloat16)

        if unrolled:
            for q in range(count):
                sample(q // samples, q % samples, q % 2)
        else:

            @pl.loop(0, n)
            def _(t):
                for i in range(samples):
                    sample(t, i, 0)

    result = call(
        body,
        (shape,) * n if unrolled else shape,
        [pltpu.VMEM((2 if unrolled else 1, 3, n * shard, length), jnp.bfloat16)],
        scalars=1,
        flops=6 * count * length * n * shard * 3 * shard,
    )(ends, *edges, *mids, above, below, weight, own_edges, own_mids)
    return result if unrolled else [result[t] for t in range(n)]


def split_dot(ones, column):
    high = column.astype(jnp.bfloat16)
    rest = column - high.astype(jnp.float32)
    middle = rest.astype(jnp.bfloat16)
    low = (rest - middle.astype(jnp.float32)).astype(jnp.bfloat16)
    lane = lax.broadcasted_iota(jnp.int32, (column.shape[0], LANES), 1)
    parts = jnp.where(lane == 0, high.astype(jnp.float32), 0.0)
    parts = jnp.where(lane == 1, middle.astype(jnp.float32), parts)
    parts = jnp.where(lane == 2, low.astype(jnp.float32), parts).astype(jnp.bfloat16)
    summed = jnp.dot(ones, parts, preferred_element_type=jnp.float32)
    return jnp.sum(summed, axis=1, keepdims=True)


def attention(chunks, weights, gain, spread, unpad, width, group):
    pieces = len(chunks)
    samples, rows, length = chunks[0].shape
    channels = rows if unpad is None else unpad.shape[1]
    heads = channels // HEAD_DIM
    keys = pieces * length
    inner = length // width - 2

    def body(*refs):
        c_refs, weight, g_ref, a_ref, b_ref = refs[:pieces], *refs[pieces : pieces + 4]
        o_ref, buf, query_buf, mixed_buf = refs[-4:]
        for i in range(samples):
            total = jnp.zeros((rows, LANES), jnp.float32)
            for c in c_refs:
                for start in range(0, length, LANES):
                    total = total + c[i, :, start : start + LANES].astype(jnp.float32)
            total = jnp.sum(total, axis=1, keepdims=True)
            mean = split_dot(b_ref[...], split_dot(a_ref[...], total)) / (keys * group)
            total = jnp.zeros((rows, LANES), jnp.float32)
            for c in c_refs:
                for start in range(0, length, LANES):
                    away = c[i, :, start : start + LANES].astype(jnp.float32) - mean
                    total = total + away * away
            total = jnp.sum(total, axis=1, keepdims=True)
            spread_of = split_dot(b_ref[...], split_dot(a_ref[...], total)) / (keys * group)
            scale = lax.rsqrt(spread_of + EPSILON) * g_ref[:, :1]
            for p, c in enumerate(c_refs):
                normed = ((c[i].astype(jnp.float32) - mean) * scale).astype(jnp.bfloat16)
                if p == 0:
                    queries = jnp.dot(
                        weight[:channels, :rows], normed, preferred_element_type=jnp.float32
                    )
                    queries = queries.astype(jnp.bfloat16).astype(jnp.float32) * HEAD_DIM ** (-0.5)
                    query_buf[...] = queries.T.astype(jnp.bfloat16)
                buf[:, p * length : (p + 1) * length] = jnp.dot(
                    weight[channels : 3 * channels, :rows],
                    normed,
                    preferred_element_type=jnp.float32,
                ).astype(jnp.bfloat16)

            for two in range(heads // 2):
                lanes = slice(two * LANES, (two + 1) * LANES)
                k_two = buf[lanes]
                v_two = buf[channels + two * LANES : channels + (two + 1) * LANES]
                q_two = query_buf[:, lanes]
                ones = jnp.ones((16, keys), jnp.bfloat16)
                pair = []
                for h in range(2):
                    cut = slice(h * HEAD_DIM, (h + 1) * HEAD_DIM)
                    scores = jnp.dot(q_two[:, cut], k_two[cut], preferred_element_type=jnp.float32)
                    below = scores - jnp.max(scores, axis=1, keepdims=True)
                    shifted = jnp.exp(below.astype(jnp.bfloat16))
                    mixed = lax.dot_general(
                        shifted,
                        jnp.concatenate([v_two[cut], ones], axis=0),
                        NT,
                        preferred_element_type=jnp.float32,
                    )
                    pair.append(mixed[:, :HEAD_DIM] / mixed[:, HEAD_DIM : HEAD_DIM + 1])
                mixed_buf[:, lanes] = jnp.concatenate(pair, axis=1).astype(jnp.bfloat16)

            own = c_refs[0][i].astype(jnp.float32).T
            if unpad is not None:
                own = jnp.dot(
                    own.astype(jnp.bfloat16),
                    refs[pieces + 4][...],
                    preferred_element_type=jnp.float32,
                )
            result = own + lax.dot_general(
                mixed_buf[...],
                weight[3 * channels :, :channels],
                NT,
                preferred_element_type=jnp.float32,
            )
            result = result.astype(jnp.bfloat16)
            o_ref[i, 0] = result[:width]
            o_ref[i, 1 + inner] = result[width : 2 * width]
            for r in range(inner):
                o_ref[i, 1 + r] = result[(2 + r) * width : (3 + r) * width]

    operands = [*chunks, weights, gain, spread.T, spread]
    if unpad is not None:
        operands.append(unpad)
    return call(
        body,
        jax.ShapeDtypeStruct((samples, length // width, width, channels), jnp.bfloat16),
        [
            pltpu.VMEM((2 * channels, keys), jnp.bfloat16),
            pltpu.VMEM((length, channels), jnp.bfloat16),
            pltpu.VMEM((length, channels), jnp.bfloat16),
        ],
    )(*operands)


def gain_column(gain):
    channels = gain.shape[1]

    def body(g_ref, o_ref):
        for start in range(0, channels, LANES):
            row = g_ref[:, start : start + LANES]
            o_ref[start : start + LANES] = jnp.broadcast_to(row, (LANES, LANES)).T

    return call(body, jax.ShapeDtypeStruct((channels, LANES), jnp.float32))(gain)


def pad_rows(values, rows, axis):
    missing = rows - values.shape[axis]
    return jnp.pad(values, [(0, missing if a == axis else 0) for a in range(values.ndim)])


def local(
    features,
    step_index,
    roster,
    time_weight,
    temb_weight,
    norm_gains,
    conv_first,
    conv_second,
    attn_weight,
    out_weight,
):
    samples, height, width, channels = features.shape
    n, planes = lax.axis_size("fsdp"), lax.axis_size("spatial")
    mine, row = lax.axis_index("fsdp"), lax.axis_index("spatial")
    group = channels // GROUPS
    kept = conv_first.shape[1]
    shard = -(-kept // 16) * 16
    length = height * width
    entries = float(length * group)
    count = n * samples
    half = planes // 2
    swap = [(i, i ^ 1) for i in range(planes)]
    ends = jnp.stack([row > 0, row < planes - 1, mine]).astype(jnp.int32)

    def ring(values):
        return [values] + [shift(values, "fsdp", j) for j in range(1, n)]

    def pad_blocks(values, axis):
        if shard == kept:
            return values
        shape = list(values.shape)
        parts = values.reshape(shape[:axis] + [shape[axis] // kept, kept] + shape[axis + 1 :])
        parts = pad_rows(parts, shard, axis + 1)
        return parts.reshape(shape[:axis] + [shape[axis] // kept * shard] + shape[axis + 1 :])

    def in_plane_stats(values):
        rows = values.shape[0] // 2
        size = 1
        while size < planes:
            other = lax.ppermute(values, "spatial", [(i, i ^ size) for i in range(planes)])
            away = values[:rows] - other[:rows]
            mean = 0.5 * (values[:rows] + other[:rows])
            squares = values[rows:] + other[rows:] + (0.5 * size * entries) * (away * away)
            values = jnp.concatenate([mean, squares], axis=0)
            size *= 2
        return values

    def in_plane(values):
        near = [values] + [shift(values, "spatial", 2 * d) for d in range(1, half)]
        far = [lax.ppermute(c, "spatial", swap) for c in near]
        back = (row - 2 * np.arange(half)) % planes
        return near + far, jnp.concatenate([back, back ^ 1]).astype(jnp.int32)

    flat = features.reshape(samples, length, channels)
    own_stats, edges = local_stats(flat, members(channels, channels, channels, group), group, width)
    edges = ring(edges)
    last, first = halo_rows(edges, width)
    above = shift_rows(last, 1)
    below = shift_rows(first, -1)
    own_stats = in_plane_stats(own_stats)
    mids = rows_message(own_stats, norm_gains[:1], entries * planes, flat, width)
    mids = ring(mids)

    wide = attn_weight.shape[1]
    part = -(-(wide + kept) // (16 * planes)) * 16
    turned = jnp.concatenate(
        [pad_blocks(attn_weight.T, 1), pad_rows(out_weight.T, n * shard, 1)], axis=0
    )
    turned = lax.dynamic_slice_in_dim(pad_rows(turned, part * planes, 0), row * part, part, 0)
    places = ((mine - np.arange(n)) % n).astype(jnp.int32)
    pieces = ring(turned[None])
    turned = place(places, pieces, 0)
    projection, from_rows = in_plane(turned)
    if wide % part or kept % part:
        turned = place(from_rows, projection, 1)
        projection = jnp.concatenate(
            [
                turned[:, :wide].reshape(n * wide, n * shard),
                turned[:, wide : wide + kept].reshape(channels, n * shard),
            ]
        )
    else:
        projection = place_weights(from_rows, projection, wide, channels)

    first_weight = pad_rows(conv_first.T, shard, 0)
    second_weight = pad_rows(pad_blocks(conv_second.T, 1), shard, 0)
    bias = time_bias(ends, step_index, roster, time_weight, temb_weight, shard, kept)

    edges, mids, own_stats, own_edges, own_mids, gain = first_conv(
        ends,
        edges,
        mids,
        above,
        below,
        first_weight,
        bias,
        same_group(shard, shard, kept, group),
        norm_gains[1:2],
        jnp.asarray(np.eye(-(-count // 8) * 8, LANES, dtype=np.float32)),
        kept,
        width,
        group,
    )

    edges = ring(edges)
    last, first = halo_columns(edges, width)
    above = shift_rows(last, 1)
    below = shift_rows(first, -1)
    own_stats = in_plane_stats(own_stats)
    mids = columns_message(own_stats, gain, entries * planes, mids)
    mids = ring(mids)
    sums = second_conv(
        ends,
        edges,
        mids,
        above,
        below,
        second_weight,
        own_edges,
        own_mids,
        samples,
        width,
    )

    own = [sums[0]] + [shift(sums[t], "fsdp", -t) for t in range(1, n)]
    own = place(((mine + np.arange(n)) % n).astype(jnp.int32), own, 1)
    chunks, _ = in_plane(own)
    gain = gain_column(pad_blocks(norm_gains[2:3], 1))
    unpad = None
    if shard != kept:
        at = np.arange(n * shard)
        at = np.where(at % shard < kept, at // shard * kept + at % shard, -1)
        unpad = jnp.asarray(at[:, None] == np.arange(channels)[None, :], jnp.bfloat16)
    return attention(
        chunks,
        projection,
        gain,
        members(n * shard, shard, kept, group),
        unpad,
        width,
        group,
    )


def shift_rows(values, step):
    count = lax.axis_size("spatial")
    pairs = [(i, i + step) for i in range(count) if 0 <= i + step < count]
    return lax.ppermute(values, "spatial", pairs)


def solution(mesh):
    in_specs = (
        P("fsdp", "spatial", None, None),
        P(),
        P(),
        P(),
        P(),
        P(),
        P(None, "fsdp"),
        P(None, "fsdp"),
        P(None, "fsdp"),
        P(None, "fsdp"),
    )
    out_specs = P("fsdp", "spatial", None, None)

    return jax.shard_map(local, mesh=mesh, in_specs=in_specs, out_specs=out_specs, check_vma=False)
```

```python
import math

import jax
import jax.numpy as jnp
import numpy as np
from jax import lax
from jax.experimental import pallas as pl
from jax.experimental.pallas import tpu as pltpu
from jax.sharding import PartitionSpec as P


HEAD_DIM = 64
GROUPS = 32
EPSILON = 1e-05
LANES = 128
HIGHEST = lax.Precision.HIGHEST


NT = (((1,), (1,)), ((), ()))


def call(body, out_shape, scratch=(), scalars=0, flops=0, near=(), limit=16):
    def run(*operands):
        near_ones = set(range(len(operands))) if near is True else set(near)
        placed = [
            pltpu.with_memory_space_constraint(x, pltpu.VMEM) if i in near_ones and i >= scalars else x
            for i, x in enumerate(operands)
        ]
        specs = [
            pl.BlockSpec(memory_space=pltpu.SMEM if i < scalars else pltpu.VMEM)
            for i in range(len(operands))
        ]
        outs = jax.tree.map(lambda _: pl.BlockSpec(memory_space=pltpu.VMEM), out_shape)
        return pl.pallas_call(
            body,
            out_shape=out_shape,
            in_specs=specs,
            out_specs=outs,
            scratch_shapes=list(scratch),
            compiler_params=pltpu.CompilerParams(vmem_limit_bytes=limit * 2**20),
            cost_estimate=pl.CostEstimate(flops=flops, transcendentals=0, bytes_accessed=0)
            if flops
            else None,
        )(*placed)

    return run


def shift(values, axis, step):
    count = lax.axis_size(axis)
    return lax.ppermute(values, axis, [(i, (i + step) % count) for i in range(count)])


def silu(v):
    half = 0.5 * v
    return half + half * jnp.tanh(half)


def own_channels(where, rows, kept, channels):
    row = lax.broadcasted_iota(jnp.int32, (rows, channels), 0)
    column = lax.broadcasted_iota(jnp.int32, (rows, channels), 1)
    chosen = (row + where * kept == column) & (row < kept)
    return jnp.where(chosen, 1.0, 0.0).astype(jnp.bfloat16)


def part_rows(row):
    at = lax.broadcasted_iota(jnp.int32, (8, row.shape[1]), 0)
    high, middle, low = three_parts(row)
    parts = jnp.where(at == 0, high, jnp.where(at == 1, middle, jnp.where(at == 2, low, 0.0)))
    return parts.astype(jnp.bfloat16)


def time_bias(ends, step_index, roster, time_weight, temb_weight, rows, kept):
    freqs, hidden = time_weight.shape
    channels = temb_weight.shape[1]
    half_len = freqs // 2
    steps = roster.shape[0]

    def column(row):
        tiles = [
            jnp.broadcast_to(row[:, start : start + LANES], (LANES, LANES)).T
            for start in range(0, row.shape[1], LANES)
        ]
        return jnp.concatenate(tiles, axis=0)[:, :1]

    def body(n_ref, i_ref, r_ref, w_ref, t_ref, o_ref):
        at = lax.broadcasted_iota(jnp.int32, (1, steps), 1)
        moment = jnp.sum(jnp.where(at == i_ref[0], r_ref[...], 0.0), axis=1, keepdims=True)
        padded = -(-half_len // LANES) * LANES
        place = lax.broadcasted_iota(jnp.int32, (1, padded), 1).astype(jnp.float32)
        angles = moment * jnp.exp(-math.log(10000.0) * place / half_len)
        time_hidden = jnp.zeros((1, hidden), jnp.float32)
        for start, wave in ((0, jnp.cos(angles)), (half_len, jnp.sin(angles))):
            time_hidden = time_hidden + jnp.sum(
                column(wave)[:half_len] * w_ref[start : start + half_len], axis=0, keepdims=True
            )
        time_hidden = time_hidden / (1.0 + jnp.exp(-time_hidden))
        summed = jnp.zeros((LANES, channels), jnp.float32)
        turned = column(time_hidden)
        for start in range(0, hidden, LANES):
            summed = summed + turned[start : start + LANES] * t_ref[start : start + LANES]
        parts = lax.dot_general(
            own_channels(n_ref[2], rows, kept, channels),
            part_rows(jnp.sum(summed, axis=0, keepdims=True)),
            NT,
            preferred_element_type=jnp.float32,
        )
        o_ref[...] = jnp.broadcast_to(jnp.sum(parts, axis=1, keepdims=True), (rows, LANES))

    return call(body, jax.ShapeDtypeStruct((rows, LANES), jnp.float32), scalars=2)(
        ends, step_index, roster[None, :], time_weight, temb_weight
    )


def group_of(rows, block, kept, width):
    index = np.arange(rows)
    group = (index // block * kept + index % block) // width
    return np.where(index % block < kept, group, -1)


def members(rows, block, kept, width):
    group = group_of(rows, block, kept, width)[:, None]
    return jnp.asarray(group == np.arange(LANES)[None, :], jnp.bfloat16)


def same_group(rows, block, kept, width):
    group = group_of(rows, block, kept, width)[:, None]
    return jnp.asarray((group == group.T) & (group >= 0), jnp.float32)


def three_parts(values):
    high = values.astype(jnp.bfloat16).astype(jnp.float32)
    rest = values - high
    middle = rest.astype(jnp.bfloat16).astype(jnp.float32)
    return high, middle, rest - middle


def group_sums(row, member):
    for dims in ((((1,), (0,)), ((), ())), NT):
        summed = lax.dot_general(
            part_rows(row), member, dims, preferred_element_type=jnp.float32
        )
        row = jnp.sum(summed, axis=0, keepdims=True)
    return row


def local_stats(features, member, width, columns):
    samples, length, channels = features.shape

    def body(x_ref, g_ref, o_ref, e_ref):
        for i in range(samples):
            e_ref[i, :columns] = x_ref[i, :columns]
            e_ref[i, columns:] = x_ref[i, length - columns :]
            v = x_ref[i].astype(jnp.float32)
            mean = group_sums(jnp.sum(v, axis=0, keepdims=True), g_ref[...]) / (length * width)
            c = v - mean
            o_ref[i : i + 1] = mean
            o_ref[samples + i : samples + i + 1] = group_sums(
                jnp.sum(c * c, axis=0, keepdims=True), g_ref[...]
            )

    shapes = (
        jax.ShapeDtypeStruct((2 * samples, channels), jnp.float32),
        jax.ShapeDtypeStruct((samples, 2 * columns, channels), jnp.bfloat16),
    )
    return call(body, shapes)(features, member)


def place_weights(where, pieces, wide, channels):
    blocks, part, depth = pieces[0].shape
    steps = wide // part

    def body(w_ref, *refs):
        for k, piece in enumerate(refs[:-1]):
            at = w_ref[k]
            for g in range(blocks):
                start = jnp.where(
                    at < steps,
                    g * wide + at * part,
                    blocks * wide + g * (channels // blocks) + (at - steps) * part,
                )
                refs[-1][pl.ds(pl.multiple_of(start, 16), part)] = piece[g]

    shape = jax.ShapeDtypeStruct((4 * channels, depth), jnp.bfloat16)
    return call(body, shape, scalars=1)(where, *pieces)


def place(where, pieces, axis, flops=0):
    first = pieces[0]
    size = first.shape[axis]
    shape = list(first.shape)
    shape[axis] = size * len(pieces)

    def body(w_ref, *refs):
        for k, piece in enumerate(refs[:-1]):
            start = pl.multiple_of(w_ref[k] * size, size)
            refs[-1][(slice(None),) * axis + (pl.ds(start, size),)] = piece[...]

    return call(body, jax.ShapeDtypeStruct(tuple(shape), first.dtype), scalars=1, flops=flops)(
        where, *pieces
    )


def norm_terms(figures, gain, entries):
    count = figures.shape[0] // 2
    return figures[:count], lax.rsqrt(figures[count:] / entries + EPSILON) * gain


TAIL = 16


def rows_message(figures, gain, entries, flat, width):
    samples, length, channels = flat.shape
    mid = length - 2 * width

    def body(p_ref, g_ref, m_ref, o_ref):
        mean, scale = norm_terms(p_ref[...], g_ref[...], entries)
        for i in range(samples):
            o_ref[i, :mid] = m_ref[i, width : width + mid]
            rows = [*three_parts(mean[i : i + 1]), *three_parts(scale[i : i + 1])]
            rows.append(jnp.zeros((TAIL - len(rows), channels), jnp.float32))
            o_ref[i, mid:] = jnp.concatenate(rows, axis=0).astype(jnp.bfloat16)

    shape = jax.ShapeDtypeStruct((samples, mid + TAIL, channels), jnp.bfloat16)
    return call(body, shape)(figures, gain, flat)


def columns_message(figures, gain, entries, mids):
    shard, wide = mids.shape

    def body(p_ref, g_ref, m_ref, o_ref):
        o_ref[:, :wide] = m_ref[...]
        terms = jnp.concatenate(norm_terms(p_ref[...], g_ref[...], entries), axis=0)
        rows = [*three_parts(terms)]
        rows.append(jnp.zeros((LANES - 3 * terms.shape[0], shard), jnp.float32))
        rows = jnp.concatenate(rows, axis=0).astype(jnp.bfloat16)
        o_ref[:, wide:] = lax.dot_general(
            identity(shard, shard), rows, NT, preferred_element_type=jnp.float32
        ).astype(jnp.bfloat16)

    shape = jax.ShapeDtypeStruct((shard, wide + LANES), jnp.bfloat16)
    return call(body, shape)(figures, gain, mids)


def identity(rows, columns):
    at = lax.broadcasted_iota(jnp.int32, (rows, columns), 0)
    same = at == lax.broadcasted_iota(jnp.int32, (rows, columns), 1)
    return jnp.where(same, 1.0, 0.0).astype(jnp.bfloat16)


def halo_rows(edges, width):
    samples, _, channels = edges[0].shape
    shape = jax.ShapeDtypeStruct((len(edges) * samples, width, channels), jnp.bfloat16)

    def body(*refs):
        for j, e in enumerate(refs[:-2]):
            refs[-2][j * samples : (j + 1) * samples] = e[:, width:]
            refs[-1][j * samples : (j + 1) * samples] = e[:, :width]

    return call(body, (shape, shape), near=True)(*edges)


def halo_columns(edges, width):
    shard, wide = edges[0].shape
    edge = 2 * width
    shape = jax.ShapeDtypeStruct((len(edges) * shard, wide // 2), jnp.bfloat16)

    def body(*refs):
        low = lax.broadcasted_iota(jnp.int32, (shard, edge), 1) < width
        for j, e in enumerate(refs[:-2]):
            rows = slice(j * shard, (j + 1) * shard)
            for p in range(wide // edge // 2):
                left = e[:, 2 * p * edge : (2 * p + 1) * edge].astype(jnp.float32)
                right = e[:, (2 * p + 1) * edge : (2 * p + 2) * edge].astype(jnp.float32)
                cut = slice(p * edge, (p + 1) * edge)
                last = jnp.where(low, pltpu.roll(left, width, axis=1), right)
                first = jnp.where(low, left, pltpu.roll(right, width, axis=1))
                refs[-2][rows, cut] = last.astype(jnp.bfloat16)
                refs[-1][rows, cut] = first.astype(jnp.bfloat16)

    return call(body, (shape, shape), near=True)(*edges)


def tap_rows(weight, row, depth):
    return jnp.concatenate(
        [weight[:, (3 * row + b) * depth : (3 * row + b + 1) * depth] for b in range(3)], axis=0
    )


def spread_column(tail, at, period):
    lane = lax.broadcasted_iota(jnp.int32, (LANES, LANES), 0)
    chosen = (lane == at) | (lane == at + period) | (lane == at + 2 * period)
    chosen = jnp.where(chosen, 1.0, 0.0).astype(jnp.bfloat16)
    return jnp.dot(tail, chosen, preferred_element_type=jnp.float32)


def tile(index, size):
    if isinstance(index, int):
        return slice(index * size, (index + 1) * size)
    return pl.ds(pl.multiple_of(index * size, LANES), size)


def column_shift(y, shard, width):
    lane = lax.broadcasted_iota(jnp.int32, (shard, LANES), 1) % width
    tiles = []
    for start in range(0, y.shape[1], LANES):
        left = y[:shard, start : start + LANES]
        right = y[2 * shard :, start : start + LANES]
        tiles.append(
            y[shard : 2 * shard, start : start + LANES]
            + jnp.where(lane > 0, pltpu.roll(left, 1, axis=1), 0.0)
            + jnp.where(lane < width - 1, pltpu.roll(right, LANES - 1, axis=1), 0.0)
        )
    return jnp.concatenate(tiles, axis=1)


def first_conv(ends, edges, mids, above, below, weight, bias, groups, gain, eye, kept, width, group):
    n = len(edges)
    samples, edge, channels = edges[0].shape
    mid = mids[0].shape[1] - TAIL
    shard = bias.shape[0]
    count = n * samples
    inner = mid // width
    length = edge + mid

    def body(*refs):
        ends_ref = refs[0]
        e_refs, m_refs = refs[1 : 1 + n], refs[1 + n : 1 + 2 * n]
        a_ref, b_ref, w_ref, t_ref, g_ref, p_ref, i_ref = refs[1 + 2 * n : 8 + 2 * n]
        eo_ref, mo_ref, so_ref, fe_ref, fm_ref, go_ref, buf, out_buf = refs[8 + 2 * n :]
        pick = own_channels(ends_ref[2], shard, kept, channels)
        parts = lax.dot_general(part_rows(p_ref[...]), pick, NT, preferred_element_type=jnp.float32)
        go_ref[...] = jnp.sum(parts, axis=0, keepdims=True)
        has_above = ends_ref[0].astype(jnp.float32)
        has_below = ends_ref[1].astype(jnp.float32)
        lane = lax.broadcasted_iota(jnp.int32, (shard, LANES), 1)
        sums = jnp.zeros((shard, LANES), jnp.float32)
        for j in range(n):
            for i in range(samples):
                q = j * samples + i
                tail = m_refs[j][i, mid:].astype(jnp.float32)
                mean = tail[0:1] + tail[1:2] + tail[2:3]
                scale = tail[3:4] + tail[4:5] + tail[5:6]

                def act(x):
                    return silu((x.astype(jnp.float32) - mean) * scale)

                e = e_refs[j][i]
                m = m_refs[j][i, :mid]
                ea = act(e).astype(jnp.bfloat16)
                buf[q % 2, :width] = (act(a_ref[q]) * has_above).astype(jnp.bfloat16)
                buf[q % 2, width : 2 * width] = ea[:width]
                buf[q % 2, 2 * width : 2 * width + mid] = act(m).astype(jnp.bfloat16)
                buf[q % 2, 2 * width + mid : 3 * width + mid] = ea[width:]
                buf[q % 2, 3 * width + mid :] = (act(b_ref[q]) * has_below).astype(jnp.bfloat16)
                y = jnp.zeros((3 * shard, length), jnp.float32)
                for a in range(3):
                    window = jnp.concatenate(
                        [
                            buf[q % 2, a * width : (a + 1) * width],
                            buf[q % 2, (a + 1 + inner) * width : (a + 2 + inner) * width],
                            buf[q % 2, (a + 1) * width : (a + 1 + inner) * width],
                        ],
                        axis=0,
                    )
                    y = y + lax.dot_general(
                        tap_rows(w_ref, a, channels), window, NT, preferred_element_type=jnp.float32
                    )
                out = column_shift(y, shard, width) + t_ref[:, :1]
                eo_ref[:, q * edge : (q + 1) * edge] = out[:, :edge].astype(jnp.bfloat16)
                mo_ref[:, q * mid : (q + 1) * mid] = out[:, edge:].astype(jnp.bfloat16)
                fe_ref[:, q * edge : (q + 1) * edge] = lax.dot_general(
                    pick, e, NT, preferred_element_type=jnp.float32
                ).astype(jnp.bfloat16)
                fm_ref[:, q * mid : (q + 1) * mid] = lax.dot_general(
                    pick, m, NT, preferred_element_type=jnp.float32
                ).astype(jnp.bfloat16)
                out_buf[q] = out
                sums = jnp.where(lane == q, jnp.sum(out, axis=1, keepdims=True), sums)
        centers = jnp.dot(g_ref[...], sums, precision=HIGHEST) / (length * group)
        sums = jnp.zeros((shard, LANES), jnp.float32)
        for q in range(count):
            c = out_buf[q] - centers[:, q : q + 1]
            sums = jnp.where(lane == q, jnp.sum(c * c, axis=1, keepdims=True), sums)
        squares = jnp.dot(g_ref[...], sums, precision=HIGHEST)
        for start, found in ((0, centers), (count, squares)):
            so_ref[start : start + count] = lax.dot_general(
                i_ref[...], found, NT, precision=HIGHEST
            )[:count]

    out_shape = (
        jax.ShapeDtypeStruct((shard, count * edge), jnp.bfloat16),
        jax.ShapeDtypeStruct((shard, count * mid), jnp.bfloat16),
        jax.ShapeDtypeStruct((2 * count, shard), jnp.float32),
        jax.ShapeDtypeStruct((shard, count * edge), jnp.bfloat16),
        jax.ShapeDtypeStruct((shard, count * mid), jnp.bfloat16),
        jax.ShapeDtypeStruct((1, shard), jnp.float32),
    )
    scratch = [
        pltpu.VMEM((2, length + 2 * width, channels), jnp.bfloat16),
        pltpu.VMEM((count, shard, length), jnp.float32),
    ]
    return call(body, out_shape, scratch, scalars=1, flops=6 * count * length * channels * 3 * shard, limit=32)(
        ends, *edges, *mids, above, below, weight, bias, groups, gain, eye
    )


def second_conv(
    ends, edges, mids, above, below, weight, own_edges, own_mids, samples, width, begin, end
):
    n = len(edges)
    shard = edges[0].shape[0]
    count = n * samples
    edge, mid = edges[0].shape[1] // count, (mids[0].shape[1] - LANES) // count
    length = edge + mid

    unrolled = n <= 4
    shape = jax.ShapeDtypeStruct((samples, shard, length), jnp.bfloat16)
    if not unrolled:
        shape = jax.ShapeDtypeStruct((n, samples, shard, length), jnp.bfloat16)

    def body(*refs):
        ends_ref = refs[0]
        e_refs, m_refs = refs[1 : 1 + n], refs[1 + n : 1 + 2 * n]
        a_ref, b_ref, w_ref, fe_ref, fm_ref = refs[1 + 2 * n : 6 + 2 * n]
        o_refs, buf = refs[6 + 2 * n : -1], refs[-1]
        low = lax.broadcasted_iota(jnp.int32, (shard, edge), 1) < width
        inside = jnp.where(low, ends_ref[0], ends_ref[1]).astype(jnp.float32)

        def sample(t, i, slot):
            for j in range(n):
                q = ((t - j) % n if unrolled else lax.rem(t - j + n, n)) * samples + i
                tail = m_refs[j][:, count * mid :]
                mean = spread_column(tail, q, 2 * count)
                scale = spread_column(tail, q + count, 2 * count)

                def act(x):
                    return silu((x - mean) * scale)

                rows = slice(j * shard, (j + 1) * shard)
                natural = pl.ds(pl.multiple_of(lax.rem(ends_ref[2] + n - j, n) * shard, 16), shard)
                half = q // 2 if unrolled else lax.div(q, 2)
                last = a_ref[rows, tile(half, edge)].astype(jnp.float32)
                first = b_ref[rows, tile(half, edge)].astype(jnp.float32)
                if unrolled:
                    odd = q % 2 == 1
                    halo = (
                        jnp.where(low, pltpu.roll(last, width, axis=1), first)
                        if odd
                        else jnp.where(low, last, pltpu.roll(first, width, axis=1))
                    )
                else:
                    halo = jnp.where(
                        lax.rem(q, 2) == 1,
                        jnp.where(low, pltpu.roll(last, width, axis=1), first),
                        jnp.where(low, last, pltpu.roll(first, width, axis=1)),
                    )
                halo = (act(halo) * inside).astype(jnp.bfloat16)
                e = act(e_refs[j][:, tile(q, edge)].astype(jnp.float32))
                m = act(m_refs[j][:, tile(q, mid)].astype(jnp.float32))
                turned = pltpu.roll(m, width, axis=1).astype(jnp.bfloat16)
                e = e.astype(jnp.bfloat16)
                m = m.astype(jnp.bfloat16)
                buf[slot, 0, natural, :edge] = jnp.where(low, halo, m)
                buf[slot, 0, natural, edge:] = jnp.where(low, e, turned)
                buf[slot, 1, natural, :edge] = e
                buf[slot, 1, natural, edge:] = m
                buf[slot, 2, natural, :edge] = jnp.where(low, m, halo)
                buf[slot, 2, natural, edge:] = jnp.where(low, turned, e)
            y = jnp.zeros((3 * shard, length), jnp.float32)
            for a in range(3):
                y = y + jnp.dot(
                    tap_rows(w_ref, a, n * shard), buf[slot, a], preferred_element_type=jnp.float32
                )
            out = column_shift(y, shard, width)
            q = t * samples + i
            target = o_refs[t - begin].at[i] if unrolled else o_refs[0].at[t, i]
            target[:, :edge] = (
                out[:, :edge] + fe_ref[:, tile(q, edge)].astype(jnp.float32)
            ).astype(jnp.bfloat16)
            target[:, edge:] = (
                out[:, edge:] + fm_ref[:, tile(q, mid)].astype(jnp.float32)
            ).astype(jnp.bfloat16)

        if unrolled:
            for q in range(begin * samples, end * samples):
                sample(q // samples, q % samples, q % 2)
        else:

            @pl.loop(0, n)
            def _(t):
                for i in range(samples):
                    sample(t, i, 0)

    result = call(
        body,
        (shape,) * (end - begin) if unrolled else shape,
        [pltpu.VMEM((2 if unrolled else 1, 3, n * shard, length), jnp.bfloat16)],
        scalars=1,
        flops=6 * count * length * n * shard * 3 * shard,
        limit=32,
    )(ends, *edges, *mids, above, below, weight, own_edges, own_mids)
    return list(result) if unrolled else [result[t] for t in range(n)]


def split_dot(ones, column):
    high = column.astype(jnp.bfloat16)
    rest = column - high.astype(jnp.float32)
    middle = rest.astype(jnp.bfloat16)
    low = (rest - middle.astype(jnp.float32)).astype(jnp.bfloat16)
    lane = lax.broadcasted_iota(jnp.int32, (column.shape[0], LANES), 1)
    parts = jnp.where(lane == 0, high.astype(jnp.float32), 0.0)
    parts = jnp.where(lane == 1, middle.astype(jnp.float32), parts)
    parts = jnp.where(lane == 2, low.astype(jnp.float32), parts).astype(jnp.bfloat16)
    summed = jnp.dot(ones, parts, preferred_element_type=jnp.float32)
    return jnp.sum(summed, axis=1, keepdims=True)


def attention(chunks, weights, gain, spread, unpad, width, group):
    pieces = len(chunks)
    samples, rows, length = chunks[0].shape
    channels = rows if unpad is None else unpad.shape[1]
    heads = channels // HEAD_DIM
    keys = pieces * length
    inner = length // width - 2

    def body(*refs):
        c_refs, weight, g_ref, a_ref, b_ref = refs[:pieces], *refs[pieces : pieces + 4]
        o_ref, buf, query_buf, mixed_buf = refs[-4:]
        for i in range(samples):
            total = jnp.zeros((rows, LANES), jnp.float32)
            for c in c_refs:
                for start in range(0, length, LANES):
                    total = total + c[i, :, start : start + LANES].astype(jnp.float32)
            total = jnp.sum(total, axis=1, keepdims=True)
            mean = split_dot(b_ref[...], split_dot(a_ref[...], total)) / (keys * group)
            total = jnp.zeros((rows, LANES), jnp.float32)
            for c in c_refs:
                for start in range(0, length, LANES):
                    away = c[i, :, start : start + LANES].astype(jnp.float32) - mean
                    total = total + away * away
            total = jnp.sum(total, axis=1, keepdims=True)
            spread_of = split_dot(b_ref[...], split_dot(a_ref[...], total)) / (keys * group)
            scale = lax.rsqrt(spread_of + EPSILON) * g_ref[:, :1]
            for p, c in enumerate(c_refs):
                normed = ((c[i].astype(jnp.float32) - mean) * scale).astype(jnp.bfloat16)
                if p == 0:
                    queries = jnp.dot(
                        weight[:channels, :rows], normed, preferred_element_type=jnp.float32
                    )
                    queries = queries.astype(jnp.bfloat16).astype(jnp.float32) * HEAD_DIM ** (-0.5)
                    query_buf[...] = queries.T.astype(jnp.bfloat16)
                buf[:, p * length : (p + 1) * length] = jnp.dot(
                    weight[channels : 3 * channels, :rows],
                    normed,
                    preferred_element_type=jnp.float32,
                ).astype(jnp.bfloat16)

            for two in range(heads // 2):
                lanes = slice(two * LANES, (two + 1) * LANES)
                k_two = buf[lanes]
                v_two = buf[channels + two * LANES : channels + (two + 1) * LANES]
                q_two = query_buf[:, lanes]
                ones = jnp.ones((16, keys), jnp.bfloat16)
                pair = []
                for h in range(2):
                    cut = slice(h * HEAD_DIM, (h + 1) * HEAD_DIM)
                    scores = jnp.dot(q_two[:, cut], k_two[cut], preferred_element_type=jnp.float32)
                    below = scores - jnp.max(scores, axis=1, keepdims=True)
                    shifted = jnp.exp(below.astype(jnp.bfloat16))
                    mixed = lax.dot_general(
                        shifted,
                        jnp.concatenate([v_two[cut], ones], axis=0),
                        NT,
                        preferred_element_type=jnp.float32,
                    )
                    pair.append(mixed[:, :HEAD_DIM] / mixed[:, HEAD_DIM : HEAD_DIM + 1])
                mixed_buf[:, lanes] = jnp.concatenate(pair, axis=1).astype(jnp.bfloat16)

            own = c_refs[0][i].astype(jnp.float32).T
            if unpad is not None:
                own = jnp.dot(
                    own.astype(jnp.bfloat16),
                    refs[pieces + 4][...],
                    preferred_element_type=jnp.float32,
                )
            result = own + lax.dot_general(
                mixed_buf[...],
                weight[3 * channels :, :channels],
                NT,
                preferred_element_type=jnp.float32,
            )
            result = result.astype(jnp.bfloat16)
            o_ref[i, 0] = result[:width]
            o_ref[i, 1 + inner] = result[width : 2 * width]
            for r in range(inner):
                o_ref[i, 1 + r] = result[(2 + r) * width : (3 + r) * width]

    operands = [*chunks, weights, gain, spread.T, spread]
    if unpad is not None:
        operands.append(unpad)
    return call(
        body,
        jax.ShapeDtypeStruct((samples, length // width, width, channels), jnp.bfloat16),
        [
            pltpu.VMEM((2 * channels, keys), jnp.bfloat16),
            pltpu.VMEM((length, channels), jnp.bfloat16),
            pltpu.VMEM((length, channels), jnp.bfloat16),
        ],
        limit=48,
    )(*operands)


def gain_column(gain):
    channels = gain.shape[1]

    def body(g_ref, o_ref):
        for start in range(0, channels, LANES):
            row = g_ref[:, start : start + LANES]
            o_ref[start : start + LANES] = jnp.broadcast_to(row, (LANES, LANES)).T

    return call(body, jax.ShapeDtypeStruct((channels, LANES), jnp.float32))(gain)


def pad_rows(values, rows, axis):
    missing = rows - values.shape[axis]
    return jnp.pad(values, [(0, missing if a == axis else 0) for a in range(values.ndim)])


def local(
    features,
    step_index,
    roster,
    time_weight,
    temb_weight,
    norm_gains,
    conv_first,
    conv_second,
    attn_weight,
    out_weight,
):
    samples, height, width, channels = features.shape
    n, planes = lax.axis_size("fsdp"), lax.axis_size("spatial")
    mine, row = lax.axis_index("fsdp"), lax.axis_index("spatial")
    group = channels // GROUPS
    kept = conv_first.shape[1]
    shard = -(-kept // 16) * 16
    length = height * width
    entries = float(length * group)
    count = n * samples
    half = planes // 2
    swap = [(i, i ^ 1) for i in range(planes)]
    ends = jnp.stack([row > 0, row < planes - 1, mine]).astype(jnp.int32)

    def ring(values):
        found = [values]
        for j in range(1, n):
            found.append(shift(values, "fsdp", j))
        return found

    def pad_blocks(values, axis):
        if shard == kept:
            return values
        shape = list(values.shape)
        parts = values.reshape(shape[:axis] + [shape[axis] // kept, kept] + shape[axis + 1 :])
        parts = pad_rows(parts, shard, axis + 1)
        return parts.reshape(shape[:axis] + [shape[axis] // kept * shard] + shape[axis + 1 :])

    def in_plane_stats(values):
        rows = values.shape[0] // 2
        size = 1
        while size < planes:
            other = lax.ppermute(values, "spatial", [(i, i ^ size) for i in range(planes)])
            away = values[:rows] - other[:rows]
            mean = 0.5 * (values[:rows] + other[:rows])
            squares = values[rows:] + other[rows:] + (0.5 * size * entries) * (away * away)
            values = jnp.concatenate([mean, squares], axis=0)
            size *= 2
        return values

    def in_plane(values):
        near = [values] + [shift(values, "spatial", 2 * d) for d in range(1, half)]
        far = [lax.ppermute(c, "spatial", swap) for c in near]
        back = (row - 2 * np.arange(half)) % planes
        return near + far, jnp.concatenate([back, back ^ 1]).astype(jnp.int32)

    flat = features.reshape(samples, length, channels)
    own_stats, edges = local_stats(flat, members(channels, channels, channels, group), group, width)
    edges = ring(edges)
    last, first = halo_rows(edges, width)
    above = shift_rows(last, 1)
    below = shift_rows(first, -1)
    own_stats = in_plane_stats(own_stats)
    mids = rows_message(own_stats, norm_gains[:1], entries * planes, flat, width)
    mids = ring(mids)

    wide = attn_weight.shape[1]
    part = -(-(wide + kept) // (16 * planes)) * 16
    turned = jnp.concatenate(
        [pad_blocks(attn_weight.T, 1), pad_rows(out_weight.T, n * shard, 1)], axis=0
    )
    turned = lax.dynamic_slice_in_dim(pad_rows(turned, part * planes, 0), row * part, part, 0)
    places = ((mine - np.arange(n)) % n).astype(jnp.int32)
    pieces = ring(turned[None])
    turned = place(places, pieces, 0)
    projection, from_rows = in_plane(turned)
    if wide % part or kept % part:
        turned = place(from_rows, projection, 1)
        projection = jnp.concatenate(
            [
                turned[:, :wide].reshape(n * wide, n * shard),
                turned[:, wide : wide + kept].reshape(channels, n * shard),
            ]
        )
    else:
        projection = place_weights(from_rows, projection, wide, channels)

    first_weight = pad_rows(conv_first.T, shard, 0)
    second_weight = pad_rows(pad_blocks(conv_second.T, 1), shard, 0)
    bias = time_bias(ends, step_index, roster, time_weight, temb_weight, shard, kept)

    edges, mids, own_stats, own_edges, own_mids, gain = first_conv(
        ends,
        edges,
        mids,
        above,
        below,
        first_weight,
        bias,
        same_group(shard, shard, kept, group),
        norm_gains[1:2],
        jnp.asarray(np.eye(-(-count // 8) * 8, LANES, dtype=np.float32)),
        kept,
        width,
        group,
    )

    edges = ring(edges)
    last, first = halo_columns(edges, width)
    above = shift_rows(last, 1)
    below = shift_rows(first, -1)
    own_stats = in_plane_stats(own_stats)
    mids = columns_message(own_stats, gain, entries * planes, mids)
    mids = ring(mids)
    own = {}
    turns = [(n // 2, n), (0, n // 2)] if n <= 4 else [(0, n)]
    for first, last in turns:
        sums = second_conv(
            ends,
            edges,
            mids,
            above,
            below,
            second_weight,
            own_edges,
            own_mids,
            samples,
            width,
            first,
            last,
        )

        for t, found in zip(range(first, last), sums):
            own[t] = shift(found, "fsdp", -t) if t > 0 else found
    own = [own[t] for t in range(n)]
    own = place(((mine + np.arange(n)) % n).astype(jnp.int32), own, 1)
    chunks, _ = in_plane(own)
    gain = gain_column(pad_blocks(norm_gains[2:3], 1))
    unpad = None
    if shard != kept:
        at = np.arange(n * shard)
        at = np.where(at % shard < kept, at // shard * kept + at % shard, -1)
        unpad = jnp.asarray(at[:, None] == np.arange(channels)[None, :], jnp.bfloat16)
    return attention(
        chunks,
        projection,
        gain,
        members(n * shard, shard, kept, group),
        unpad,
        width,
        group,
    )


def shift_rows(values, step):
    count = lax.axis_size("spatial")
    pairs = [(i, i + step) for i in range(count) if 0 <= i + step < count]
    return lax.ppermute(values, "spatial", pairs)


def solution(mesh):
    in_specs = (
        P("fsdp", "spatial", None, None),
        P(),
        P(),
        P(),
        P(),
        P(),
        P(None, "fsdp"),
        P(None, "fsdp"),
        P(None, "fsdp"),
        P(None, "fsdp"),
    )
    out_specs = P("fsdp", "spatial", None, None)

    return jax.shard_map(local, mesh=mesh, in_specs=in_specs, out_specs=out_specs, check_vma=False)
```

```python
import math

import jax
import jax.numpy as jnp
import numpy as np
from jax import lax
from jax.experimental import pallas as pl
from jax.experimental.pallas import tpu as pltpu
from jax.sharding import PartitionSpec as P


HEAD_DIM = 64
GROUPS = 32
EPSILON = 1e-05
LANES = 128
HIGHEST = lax.Precision.HIGHEST


NT = (((1,), (1,)), ((), ()))


def call(body, out_shape, scratch=(), scalars=0, flops=0, near=(), far=(), limit=16):
    def run(*operands):
        near_ones = set(range(len(operands))) if near is True else set(near)
        placed = [
            pltpu.with_memory_space_constraint(x, pltpu.VMEM) if i in near_ones and i >= scalars else x
            for i, x in enumerate(operands)
        ]
        for i in far:
            placed[i] = pltpu.with_memory_space_constraint(placed[i], pltpu.HBM)
        specs = [
            pl.BlockSpec(memory_space=pltpu.SMEM if i < scalars else pltpu.VMEM)
            for i in range(len(operands))
        ]
        outs = jax.tree.map(lambda _: pl.BlockSpec(memory_space=pltpu.VMEM), out_shape)
        return pl.pallas_call(
            body,
            out_shape=out_shape,
            in_specs=specs,
            out_specs=outs,
            scratch_shapes=list(scratch),
            compiler_params=pltpu.CompilerParams(vmem_limit_bytes=limit * 2**20),
            cost_estimate=pl.CostEstimate(flops=flops, transcendentals=0, bytes_accessed=0)
            if flops
            else None,
        )(*placed)

    return run


def shift(values, axis, step):
    count = lax.axis_size(axis)
    return lax.ppermute(values, axis, [(i, (i + step) % count) for i in range(count)])


def silu(v):
    half = 0.5 * v
    return half + half * jnp.tanh(half)


def own_channels(where, rows, kept, channels):
    row = lax.broadcasted_iota(jnp.int32, (rows, channels), 0)
    column = lax.broadcasted_iota(jnp.int32, (rows, channels), 1)
    chosen = (row + where * kept == column) & (row < kept)
    return jnp.where(chosen, 1.0, 0.0).astype(jnp.bfloat16)


def part_rows(row):
    at = lax.broadcasted_iota(jnp.int32, (8, row.shape[1]), 0)
    high, middle, low = three_parts(row)
    parts = jnp.where(at == 0, high, jnp.where(at == 1, middle, jnp.where(at == 2, low, 0.0)))
    return parts.astype(jnp.bfloat16)


def time_bias(ends, step_index, roster, time_weight, temb_weight, rows, kept):
    freqs, hidden = time_weight.shape
    channels = temb_weight.shape[1]
    half_len = freqs // 2
    steps = roster.shape[0]

    def column(row):
        tiles = [
            jnp.broadcast_to(row[:, start : start + LANES], (LANES, LANES)).T
            for start in range(0, row.shape[1], LANES)
        ]
        return jnp.concatenate(tiles, axis=0)[:, :1]

    def body(n_ref, i_ref, r_ref, w_ref, t_ref, o_ref):
        at = lax.broadcasted_iota(jnp.int32, (1, steps), 1)
        moment = jnp.sum(jnp.where(at == i_ref[0], r_ref[...], 0.0), axis=1, keepdims=True)
        padded = -(-half_len // LANES) * LANES
        place = lax.broadcasted_iota(jnp.int32, (1, padded), 1).astype(jnp.float32)
        angles = moment * jnp.exp(-math.log(10000.0) * place / half_len)
        time_hidden = jnp.zeros((1, hidden), jnp.float32)
        for start, wave in ((0, jnp.cos(angles)), (half_len, jnp.sin(angles))):
            time_hidden = time_hidden + jnp.sum(
                column(wave)[:half_len] * w_ref[start : start + half_len], axis=0, keepdims=True
            )
        time_hidden = time_hidden / (1.0 + jnp.exp(-time_hidden))
        summed = jnp.zeros((LANES, channels), jnp.float32)
        turned = column(time_hidden)
        for start in range(0, hidden, LANES):
            summed = summed + turned[start : start + LANES] * t_ref[start : start + LANES]
        parts = lax.dot_general(
            own_channels(n_ref[2], rows, kept, channels),
            part_rows(jnp.sum(summed, axis=0, keepdims=True)),
            NT,
            preferred_element_type=jnp.float32,
        )
        o_ref[...] = jnp.broadcast_to(jnp.sum(parts, axis=1, keepdims=True), (rows, LANES))

    shape = jax.ShapeDtypeStruct((rows, LANES), jnp.float32)
    return call(body, shape, scalars=2, far=(3, 4))(
        ends, step_index, roster[None, :], time_weight, temb_weight
    )


def group_of(rows, block, kept, width):
    index = np.arange(rows)
    group = (index // block * kept + index % block) // width
    return np.where(index % block < kept, group, -1)


def members(rows, block, kept, width):
    group = group_of(rows, block, kept, width)[:, None]
    return jnp.asarray(group == np.arange(LANES)[None, :], jnp.bfloat16)


def same_group(rows, block, kept, width):
    group = group_of(rows, block, kept, width)[:, None]
    return jnp.asarray((group == group.T) & (group >= 0), jnp.float32)


def three_parts(values):
    high = values.astype(jnp.bfloat16).astype(jnp.float32)
    rest = values - high
    middle = rest.astype(jnp.bfloat16).astype(jnp.float32)
    return high, middle, rest - middle


def group_sums(row, member):
    for dims in ((((1,), (0,)), ((), ())), NT):
        summed = lax.dot_general(
            part_rows(row), member, dims, preferred_element_type=jnp.float32
        )
        row = jnp.sum(summed, axis=0, keepdims=True)
    return row


def local_stats(features, member, width):
    samples, length, channels = features.shape

    def body(x_ref, g_ref, o_ref):
        for i in range(samples):
            v = x_ref[i].astype(jnp.float32)
            mean = group_sums(jnp.sum(v, axis=0, keepdims=True), g_ref[...]) / (length * width)
            c = v - mean
            o_ref[i : i + 1] = mean
            o_ref[samples + i : samples + i + 1] = group_sums(
                jnp.sum(c * c, axis=0, keepdims=True), g_ref[...]
            )

    return call(body, jax.ShapeDtypeStruct((2 * samples, channels), jnp.float32))(features, member)


def place_weights(where, pieces, wide, channels):
    blocks, part, depth = pieces[0].shape
    steps = wide // part

    def body(w_ref, *refs):
        for k, piece in enumerate(refs[:-1]):
            at = w_ref[k]
            for g in range(blocks):
                start = jnp.where(
                    at < steps,
                    g * wide + at * part,
                    blocks * wide + g * (channels // blocks) + (at - steps) * part,
                )
                refs[-1][pl.ds(pl.multiple_of(start, 16), part)] = piece[g]

    shape = jax.ShapeDtypeStruct((4 * channels, depth), jnp.bfloat16)
    return call(body, shape, scalars=1)(where, *pieces)


def place(where, pieces, axis, flops=0):
    first = pieces[0]
    size = first.shape[axis]
    shape = list(first.shape)
    shape[axis] = size * len(pieces)

    def body(w_ref, *refs):
        for k, piece in enumerate(refs[:-1]):
            start = pl.multiple_of(w_ref[k] * size, size)
            refs[-1][(slice(None),) * axis + (pl.ds(start, size),)] = piece[...]

    return call(body, jax.ShapeDtypeStruct(tuple(shape), first.dtype), scalars=1, flops=flops)(
        where, *pieces
    )


def norm_terms(figures, gain, entries):
    count = figures.shape[0] // 2
    return figures[:count], lax.rsqrt(figures[count:] / entries + EPSILON) * gain


TAIL = 16


def rows_message(figures, gain, entries, flat, width):
    samples, length, channels = flat.shape
    mid = length - 2 * width

    def body(p_ref, g_ref, m_ref, o_ref):
        mean, scale = norm_terms(p_ref[...], g_ref[...], entries)
        for i in range(samples):
            o_ref[i, :mid] = m_ref[i, width : width + mid]
            rows = [*three_parts(mean[i : i + 1]), *three_parts(scale[i : i + 1])]
            rows.append(jnp.zeros((TAIL - len(rows), channels), jnp.float32))
            o_ref[i, mid:] = jnp.concatenate(rows, axis=0).astype(jnp.bfloat16)

    shape = jax.ShapeDtypeStruct((samples, mid + TAIL, channels), jnp.bfloat16)
    return call(body, shape)(figures, gain, flat)


def columns_message(figures, gain, entries, mids):
    shard, wide = mids.shape

    def body(p_ref, g_ref, m_ref, o_ref):
        o_ref[:, :wide] = m_ref[...]
        terms = jnp.concatenate(norm_terms(p_ref[...], g_ref[...], entries), axis=0)
        rows = [*three_parts(terms)]
        rows.append(jnp.zeros((LANES - 3 * terms.shape[0], shard), jnp.float32))
        rows = jnp.concatenate(rows, axis=0).astype(jnp.bfloat16)
        o_ref[:, wide:] = lax.dot_general(
            identity(shard, shard), rows, NT, preferred_element_type=jnp.float32
        ).astype(jnp.bfloat16)

    shape = jax.ShapeDtypeStruct((shard, wide + LANES), jnp.bfloat16)
    return call(body, shape)(figures, gain, mids)


def identity(rows, columns):
    at = lax.broadcasted_iota(jnp.int32, (rows, columns), 0)
    same = at == lax.broadcasted_iota(jnp.int32, (rows, columns), 1)
    return jnp.where(same, 1.0, 0.0).astype(jnp.bfloat16)


def halo_rows(edges, width):
    samples, _, channels = edges[0].shape
    shape = jax.ShapeDtypeStruct((len(edges) * samples, width, channels), jnp.bfloat16)

    def body(*refs):
        for j, e in enumerate(refs[:-2]):
            refs[-2][j * samples : (j + 1) * samples] = e[:, width:]
            refs[-1][j * samples : (j + 1) * samples] = e[:, :width]

    return call(body, (shape, shape), near=True)(*edges)


def halo_columns(edges, width):
    shard, wide = edges[0].shape
    edge = 2 * width
    shape = jax.ShapeDtypeStruct((len(edges) * shard, wide // 2), jnp.bfloat16)

    def body(*refs):
        low = lax.broadcasted_iota(jnp.int32, (shard, edge), 1) < width
        for j, e in enumerate(refs[:-2]):
            rows = slice(j * shard, (j + 1) * shard)
            for p in range(wide // edge // 2):
                left = e[:, 2 * p * edge : (2 * p + 1) * edge].astype(jnp.float32)
                right = e[:, (2 * p + 1) * edge : (2 * p + 2) * edge].astype(jnp.float32)
                cut = slice(p * edge, (p + 1) * edge)
                last = jnp.where(low, pltpu.roll(left, width, axis=1), right)
                first = jnp.where(low, left, pltpu.roll(right, width, axis=1))
                refs[-2][rows, cut] = last.astype(jnp.bfloat16)
                refs[-1][rows, cut] = first.astype(jnp.bfloat16)

    return call(body, (shape, shape), near=True)(*edges)


def tap_rows(weight, row, depth):
    return jnp.concatenate(
        [weight[:, (3 * row + b) * depth : (3 * row + b + 1) * depth] for b in range(3)], axis=0
    )


def spread_column(tail, at, period):
    lane = lax.broadcasted_iota(jnp.int32, (LANES, LANES), 0)
    chosen = (lane == at) | (lane == at + period) | (lane == at + 2 * period)
    chosen = jnp.where(chosen, 1.0, 0.0).astype(jnp.bfloat16)
    return jnp.dot(tail, chosen, preferred_element_type=jnp.float32)


def tile(index, size):
    if isinstance(index, int):
        return slice(index * size, (index + 1) * size)
    return pl.ds(pl.multiple_of(index * size, LANES), size)


def column_shift(y, shard, width):
    lane = lax.broadcasted_iota(jnp.int32, (shard, LANES), 1) % width
    tiles = []
    for start in range(0, y.shape[1], LANES):
        left = y[:shard, start : start + LANES]
        right = y[2 * shard :, start : start + LANES]
        tiles.append(
            y[shard : 2 * shard, start : start + LANES]
            + jnp.where(lane > 0, pltpu.roll(left, 1, axis=1), 0.0)
            + jnp.where(lane < width - 1, pltpu.roll(right, LANES - 1, axis=1), 0.0)
        )
    return jnp.concatenate(tiles, axis=1)


def first_conv(ends, edges, mids, above, below, weight, bias, groups, gain, eye, kept, width, group):
    n = len(edges)
    samples, edge, channels = edges[0].shape
    mid = mids[0].shape[1] - TAIL
    shard = bias.shape[0]
    count = n * samples
    inner = mid // width
    length = edge + mid

    def body(*refs):
        ends_ref = refs[0]
        e_refs, m_refs = refs[1 : 1 + n], refs[1 + n : 1 + 2 * n]
        a_ref, b_ref, w_ref, t_ref, g_ref, p_ref, i_ref = refs[1 + 2 * n : 8 + 2 * n]
        eo_ref, mo_ref, so_ref, fe_ref, fm_ref, go_ref, buf, out_buf = refs[8 + 2 * n :]
        pick = own_channels(ends_ref[2], shard, kept, channels)
        parts = lax.dot_general(part_rows(p_ref[...]), pick, NT, preferred_element_type=jnp.float32)
        go_ref[...] = jnp.sum(parts, axis=0, keepdims=True)
        has_above = ends_ref[0].astype(jnp.float32)
        has_below = ends_ref[1].astype(jnp.float32)
        lane = lax.broadcasted_iota(jnp.int32, (shard, LANES), 1)
        sums = jnp.zeros((shard, LANES), jnp.float32)
        for j in range(n):
            for i in range(samples):
                q = j * samples + i
                tail = m_refs[j][i, mid:].astype(jnp.float32)
                mean = tail[0:1] + tail[1:2] + tail[2:3]
                scale = tail[3:4] + tail[4:5] + tail[5:6]

                def act(x):
                    return silu((x.astype(jnp.float32) - mean) * scale)

                e = e_refs[j][i]
                m = m_refs[j][i, :mid]
                ea = act(e).astype(jnp.bfloat16)
                buf[q % 2, :width] = (act(a_ref[q]) * has_above).astype(jnp.bfloat16)
                buf[q % 2, width : 2 * width] = ea[:width]
                buf[q % 2, 2 * width : 2 * width + mid] = act(m).astype(jnp.bfloat16)
                buf[q % 2, 2 * width + mid : 3 * width + mid] = ea[width:]
                buf[q % 2, 3 * width + mid :] = (act(b_ref[q]) * has_below).astype(jnp.bfloat16)
                y = jnp.zeros((3 * shard, length), jnp.float32)
                for a in range(3):
                    window = jnp.concatenate(
                        [
                            buf[q % 2, a * width : (a + 1) * width],
                            buf[q % 2, (a + 1 + inner) * width : (a + 2 + inner) * width],
                            buf[q % 2, (a + 1) * width : (a + 1 + inner) * width],
                        ],
                        axis=0,
                    )
                    y = y + lax.dot_general(
                        tap_rows(w_ref, a, channels), window, NT, preferred_element_type=jnp.float32
                    )
                out = column_shift(y, shard, width) + t_ref[:, :1]
                eo_ref[:, q * edge : (q + 1) * edge] = out[:, :edge].astype(jnp.bfloat16)
                mo_ref[:, q * mid : (q + 1) * mid] = out[:, edge:].astype(jnp.bfloat16)
                fe_ref[:, q * edge : (q + 1) * edge] = lax.dot_general(
                    pick, e, NT, preferred_element_type=jnp.float32
                ).astype(jnp.bfloat16)
                fm_ref[:, q * mid : (q + 1) * mid] = lax.dot_general(
                    pick, m, NT, preferred_element_type=jnp.float32
                ).astype(jnp.bfloat16)
                out_buf[q] = out
                sums = jnp.where(lane == q, jnp.sum(out, axis=1, keepdims=True), sums)
        centers = jnp.dot(g_ref[...], sums, precision=HIGHEST) / (length * group)
        sums = jnp.zeros((shard, LANES), jnp.float32)
        for q in range(count):
            c = out_buf[q] - centers[:, q : q + 1]
            sums = jnp.where(lane == q, jnp.sum(c * c, axis=1, keepdims=True), sums)
        squares = jnp.dot(g_ref[...], sums, precision=HIGHEST)
        for start, found in ((0, centers), (count, squares)):
            so_ref[start : start + count] = lax.dot_general(
                i_ref[...], found, NT, precision=HIGHEST
            )[:count]

    out_shape = (
        jax.ShapeDtypeStruct((shard, count * edge), jnp.bfloat16),
        jax.ShapeDtypeStruct((shard, count * mid), jnp.bfloat16),
        jax.ShapeDtypeStruct((2 * count, shard), jnp.float32),
        jax.ShapeDtypeStruct((shard, count * edge), jnp.bfloat16),
        jax.ShapeDtypeStruct((shard, count * mid), jnp.bfloat16),
        jax.ShapeDtypeStruct((1, shard), jnp.float32),
    )
    scratch = [
        pltpu.VMEM((2, length + 2 * width, channels), jnp.bfloat16),
        pltpu.VMEM((count, shard, length), jnp.float32),
    ]
    return call(body, out_shape, scratch, scalars=1, flops=6 * count * length * channels * 3 * shard, limit=32)(
        ends, *edges, *mids, above, below, weight, bias, groups, gain, eye
    )


def second_conv(
    ends, edges, mids, above, below, weight, own_edges, own_mids, samples, width, begin, end
):
    n = len(edges)
    shard = edges[0].shape[0]
    count = n * samples
    edge, mid = edges[0].shape[1] // count, (mids[0].shape[1] - LANES) // count
    length = edge + mid

    unrolled = n <= 4
    shape = jax.ShapeDtypeStruct((samples, shard, length), jnp.bfloat16)
    if not unrolled:
        shape = jax.ShapeDtypeStruct((n, samples, shard, length), jnp.bfloat16)

    def body(*refs):
        ends_ref = refs[0]
        e_refs, m_refs = refs[1 : 1 + n], refs[1 + n : 1 + 2 * n]
        a_ref, b_ref, w_ref, fe_ref, fm_ref = refs[1 + 2 * n : 6 + 2 * n]
        o_refs, buf = refs[6 + 2 * n : -1], refs[-1]
        low = lax.broadcasted_iota(jnp.int32, (shard, edge), 1) < width
        inside = jnp.where(low, ends_ref[0], ends_ref[1]).astype(jnp.float32)

        def sample(t, i, slot):
            for j in range(n):
                q = ((t - j) % n if unrolled else lax.rem(t - j + n, n)) * samples + i
                tail = m_refs[j][:, count * mid :]
                mean = spread_column(tail, q, 2 * count)
                scale = spread_column(tail, q + count, 2 * count)

                def act(x):
                    return silu((x - mean) * scale)

                rows = slice(j * shard, (j + 1) * shard)
                natural = pl.ds(pl.multiple_of(lax.rem(ends_ref[2] + n - j, n) * shard, 16), shard)
                half = q // 2 if unrolled else lax.div(q, 2)
                last = a_ref[rows, tile(half, edge)].astype(jnp.float32)
                first = b_ref[rows, tile(half, edge)].astype(jnp.float32)
                if unrolled:
                    odd = q % 2 == 1
                    halo = (
                        jnp.where(low, pltpu.roll(last, width, axis=1), first)
                        if odd
                        else jnp.where(low, last, pltpu.roll(first, width, axis=1))
                    )
                else:
                    halo = jnp.where(
                        lax.rem(q, 2) == 1,
                        jnp.where(low, pltpu.roll(last, width, axis=1), first),
                        jnp.where(low, last, pltpu.roll(first, width, axis=1)),
                    )
                halo = (act(halo) * inside).astype(jnp.bfloat16)
                e = act(e_refs[j][:, tile(q, edge)].astype(jnp.float32))
                m = act(m_refs[j][:, tile(q, mid)].astype(jnp.float32))
                turned = pltpu.roll(m, width, axis=1).astype(jnp.bfloat16)
                e = e.astype(jnp.bfloat16)
                m = m.astype(jnp.bfloat16)
                buf[slot, 0, natural, :edge] = jnp.where(low, halo, m)
                buf[slot, 0, natural, edge:] = jnp.where(low, e, turned)
                buf[slot, 1, natural, :edge] = e
                buf[slot, 1, natural, edge:] = m
                buf[slot, 2, natural, :edge] = jnp.where(low, m, halo)
                buf[slot, 2, natural, edge:] = jnp.where(low, turned, e)
            y = jnp.zeros((3 * shard, length), jnp.float32)
            for a in range(3):
                y = y + jnp.dot(
                    tap_rows(w_ref, a, n * shard), buf[slot, a], preferred_element_type=jnp.float32
                )
            out = column_shift(y, shard, width)
            q = t * samples + i
            target = o_refs[t - begin].at[i] if unrolled else o_refs[0].at[t, i]
            target[:, :edge] = (
                out[:, :edge] + fe_ref[:, tile(q, edge)].astype(jnp.float32)
            ).astype(jnp.bfloat16)
            target[:, edge:] = (
                out[:, edge:] + fm_ref[:, tile(q, mid)].astype(jnp.float32)
            ).astype(jnp.bfloat16)

        if unrolled:
            for q in range(begin * samples, end * samples):
                sample(q // samples, q % samples, q % 2)
        else:

            @pl.loop(0, n)
            def _(t):
                for i in range(samples):
                    sample(t, i, 0)

    result = call(
        body,
        (shape,) * (end - begin) if unrolled else shape,
        [pltpu.VMEM((2 if unrolled else 1, 3, n * shard, length), jnp.bfloat16)],
        scalars=1,
        flops=6 * count * length * n * shard * 3 * shard,
        limit=32,
    )(ends, *edges, *mids, above, below, weight, own_edges, own_mids)
    return list(result) if unrolled else [result[t] for t in range(n)]


def split_dot(ones, column):
    high = column.astype(jnp.bfloat16)
    rest = column - high.astype(jnp.float32)
    middle = rest.astype(jnp.bfloat16)
    low = (rest - middle.astype(jnp.float32)).astype(jnp.bfloat16)
    lane = lax.broadcasted_iota(jnp.int32, (column.shape[0], LANES), 1)
    parts = jnp.where(lane == 0, high.astype(jnp.float32), 0.0)
    parts = jnp.where(lane == 1, middle.astype(jnp.float32), parts)
    parts = jnp.where(lane == 2, low.astype(jnp.float32), parts).astype(jnp.bfloat16)
    summed = jnp.dot(ones, parts, preferred_element_type=jnp.float32)
    return jnp.sum(summed, axis=1, keepdims=True)


def attention(chunks, weights, gain, spread, unpad, width, group):
    pieces = len(chunks)
    samples, rows, length = chunks[0].shape
    channels = rows if unpad is None else unpad.shape[1]
    heads = channels // HEAD_DIM
    keys = pieces * length
    inner = length // width - 2

    def body(*refs):
        c_refs, weight, g_ref, a_ref, b_ref = refs[:pieces], *refs[pieces : pieces + 4]
        o_ref, buf, query_buf, mixed_buf = refs[-4:]
        for i in range(samples):
            total = jnp.zeros((rows, LANES), jnp.float32)
            for c in c_refs:
                for start in range(0, length, LANES):
                    total = total + c[i, :, start : start + LANES].astype(jnp.float32)
            total = jnp.sum(total, axis=1, keepdims=True)
            mean = split_dot(b_ref[...], split_dot(a_ref[...], total)) / (keys * group)
            total = jnp.zeros((rows, LANES), jnp.float32)
            for c in c_refs:
                for start in range(0, length, LANES):
                    away = c[i, :, start : start + LANES].astype(jnp.float32) - mean
                    total = total + away * away
            total = jnp.sum(total, axis=1, keepdims=True)
            spread_of = split_dot(b_ref[...], split_dot(a_ref[...], total)) / (keys * group)
            scale = lax.rsqrt(spread_of + EPSILON) * g_ref[:, :1]
            for p, c in enumerate(c_refs):
                normed = ((c[i].astype(jnp.float32) - mean) * scale).astype(jnp.bfloat16)
                if p == 0:
                    queries = jnp.dot(
                        weight[:channels, :rows], normed, preferred_element_type=jnp.float32
                    )
                    queries = queries.astype(jnp.bfloat16).astype(jnp.float32) * HEAD_DIM ** (-0.5)
                    query_buf[...] = queries.T.astype(jnp.bfloat16)
                buf[:, p * length : (p + 1) * length] = jnp.dot(
                    weight[channels : 3 * channels, :rows],
                    normed,
                    preferred_element_type=jnp.float32,
                ).astype(jnp.bfloat16)

            for two in range(heads // 2):
                lanes = slice(two * LANES, (two + 1) * LANES)
                k_two = buf[lanes]
                v_two = buf[channels + two * LANES : channels + (two + 1) * LANES]
                q_two = query_buf[:, lanes]
                ones = jnp.ones((16, keys), jnp.bfloat16)
                pair = []
                for h in range(2):
                    cut = slice(h * HEAD_DIM, (h + 1) * HEAD_DIM)
                    scores = jnp.dot(q_two[:, cut], k_two[cut], preferred_element_type=jnp.float32)
                    below = scores - jnp.max(scores, axis=1, keepdims=True)
                    shifted = jnp.exp(below.astype(jnp.bfloat16))
                    mixed = lax.dot_general(
                        shifted,
                        jnp.concatenate([v_two[cut], ones], axis=0),
                        NT,
                        preferred_element_type=jnp.float32,
                    )
                    pair.append(mixed[:, :HEAD_DIM] / mixed[:, HEAD_DIM : HEAD_DIM + 1])
                mixed_buf[:, lanes] = jnp.concatenate(pair, axis=1).astype(jnp.bfloat16)

            own = c_refs[0][i].astype(jnp.float32).T
            if unpad is not None:
                own = jnp.dot(
                    own.astype(jnp.bfloat16),
                    refs[pieces + 4][...],
                    preferred_element_type=jnp.float32,
                )
            result = own + lax.dot_general(
                mixed_buf[...],
                weight[3 * channels :, :channels],
                NT,
                preferred_element_type=jnp.float32,
            )
            result = result.astype(jnp.bfloat16)
            o_ref[i, 0] = result[:width]
            o_ref[i, 1 + inner] = result[width : 2 * width]
            for r in range(inner):
                o_ref[i, 1 + r] = result[(2 + r) * width : (3 + r) * width]

    operands = [*chunks, weights, gain, spread.T, spread]
    if unpad is not None:
        operands.append(unpad)
    return call(
        body,
        jax.ShapeDtypeStruct((samples, length // width, width, channels), jnp.bfloat16),
        [
            pltpu.VMEM((2 * channels, keys), jnp.bfloat16),
            pltpu.VMEM((length, channels), jnp.bfloat16),
            pltpu.VMEM((length, channels), jnp.bfloat16),
        ],
        limit=48,
    )(*operands)


def gain_column(gain):
    channels = gain.shape[1]

    def body(g_ref, o_ref):
        for start in range(0, channels, LANES):
            row = g_ref[:, start : start + LANES]
            o_ref[start : start + LANES] = jnp.broadcast_to(row, (LANES, LANES)).T

    return call(body, jax.ShapeDtypeStruct((channels, LANES), jnp.float32))(gain)


def pad_rows(values, rows, axis):
    missing = rows - values.shape[axis]
    return jnp.pad(values, [(0, missing if a == axis else 0) for a in range(values.ndim)])


def local(
    features,
    step_index,
    roster,
    time_weight,
    temb_weight,
    norm_gains,
    conv_first,
    conv_second,
    attn_weight,
    out_weight,
):
    samples, height, width, channels = features.shape
    n, planes = lax.axis_size("fsdp"), lax.axis_size("spatial")
    mine, row = lax.axis_index("fsdp"), lax.axis_index("spatial")
    group = channels // GROUPS
    kept = conv_first.shape[1]
    shard = -(-kept // 16) * 16
    length = height * width
    entries = float(length * group)
    count = n * samples
    half = planes // 2
    swap = [(i, i ^ 1) for i in range(planes)]
    ends = jnp.stack([row > 0, row < planes - 1, mine]).astype(jnp.int32)

    def ring(values):
        found = [values]
        for j in range(1, n):
            found.append(shift(values, "fsdp", j))
        return found

    def pad_blocks(values, axis):
        if shard == kept:
            return values
        shape = list(values.shape)
        parts = values.reshape(shape[:axis] + [shape[axis] // kept, kept] + shape[axis + 1 :])
        parts = pad_rows(parts, shard, axis + 1)
        return parts.reshape(shape[:axis] + [shape[axis] // kept * shard] + shape[axis + 1 :])

    def in_plane_stats(values):
        rows = values.shape[0] // 2
        size = 1
        while size < planes:
            other = lax.ppermute(values, "spatial", [(i, i ^ size) for i in range(planes)])
            away = values[:rows] - other[:rows]
            mean = 0.5 * (values[:rows] + other[:rows])
            squares = values[rows:] + other[rows:] + (0.5 * size * entries) * (away * away)
            values = jnp.concatenate([mean, squares], axis=0)
            size *= 2
        return values

    def in_plane(values):
        near = [values] + [shift(values, "spatial", 2 * d) for d in range(1, half)]
        far = [lax.ppermute(c, "spatial", swap) for c in near]
        back = (row - 2 * np.arange(half)) % planes
        return near + far, jnp.concatenate([back, back ^ 1]).astype(jnp.int32)

    flat = features.reshape(samples, length, channels)
    edges = ring(jnp.concatenate([flat[:, :width], flat[:, length - width :]], axis=1))
    own_stats = local_stats(flat, members(channels, channels, channels, group), group)
    last, first = halo_rows(edges, width)
    above = shift_rows(last, 1)
    below = shift_rows(first, -1)
    own_stats = in_plane_stats(own_stats)
    mids = rows_message(own_stats, norm_gains[:1], entries * planes, flat, width)
    mids = ring(mids)

    wide = attn_weight.shape[1]
    part = -(-(wide + kept) // (16 * planes)) * 16
    turned = jnp.concatenate(
        [pad_blocks(attn_weight.T, 1), pad_rows(out_weight.T, n * shard, 1)], axis=0
    )
    turned = lax.dynamic_slice_in_dim(pad_rows(turned, part * planes, 0), row * part, part, 0)
    places = ((mine - np.arange(n)) % n).astype(jnp.int32)
    pieces = ring(turned[None])
    turned = place(places, pieces, 0)
    projection, from_rows = in_plane(turned)
    if wide % part or kept % part:
        turned = place(from_rows, projection, 1)
        projection = jnp.concatenate(
            [
                turned[:, :wide].reshape(n * wide, n * shard),
                turned[:, wide : wide + kept].reshape(channels, n * shard),
            ]
        )
    else:
        projection = place_weights(from_rows, projection, wide, channels)

    first_weight = pad_rows(conv_first.T, shard, 0)
    second_weight = pad_rows(pad_blocks(conv_second.T, 1), shard, 0)
    bias = time_bias(ends, step_index, roster, time_weight, temb_weight, shard, kept)

    edges, mids, own_stats, own_edges, own_mids, gain = first_conv(
        ends,
        edges,
        mids,
        above,
        below,
        first_weight,
        bias,
        same_group(shard, shard, kept, group),
        norm_gains[1:2],
        jnp.asarray(np.eye(-(-count // 8) * 8, LANES, dtype=np.float32)),
        kept,
        width,
        group,
    )

    edges = ring(edges)
    last, first = halo_columns(edges, width)
    above = shift_rows(last, 1)
    below = shift_rows(first, -1)
    own_stats = in_plane_stats(own_stats)
    mids = columns_message(own_stats, gain, entries * planes, mids)
    mids = ring(mids)
    own = {}
    turns = [(n // 2, n), (0, n // 2)] if n <= 4 else [(0, n)]
    for first, last in turns:
        sums = second_conv(
            ends,
            edges,
            mids,
            above,
            below,
            second_weight,
            own_edges,
            own_mids,
            samples,
            width,
            first,
            last,
        )

        for t, found in zip(range(first, last), sums):
            own[t] = shift(found, "fsdp", -t) if t > 0 else found
    own = [own[t] for t in range(n)]
    own = place(((mine + np.arange(n)) % n).astype(jnp.int32), own, 1)
    chunks, _ = in_plane(own)
    gain = gain_column(pad_blocks(norm_gains[2:3], 1))
    unpad = None
    if shard != kept:
        at = np.arange(n * shard)
        at = np.where(at % shard < kept, at // shard * kept + at % shard, -1)
        unpad = jnp.asarray(at[:, None] == np.arange(channels)[None, :], jnp.bfloat16)
    return attention(
        chunks,
        projection,
        gain,
        members(n * shard, shard, kept, group),
        unpad,
        width,
        group,
    )


def shift_rows(values, step):
    count = lax.axis_size("spatial")
    pairs = [(i, i + step) for i in range(count) if 0 <= i + step < count]
    return lax.ppermute(values, "spatial", pairs)


def solution(mesh):
    in_specs = (
        P("fsdp", "spatial", None, None),
        P(),
        P(),
        P(),
        P(),
        P(),
        P(None, "fsdp"),
        P(None, "fsdp"),
        P(None, "fsdp"),
        P(None, "fsdp"),
    )
    out_specs = P("fsdp", "spatial", None, None)

    return jax.shard_map(local, mesh=mesh, in_specs=in_specs, out_specs=out_specs, check_vma=False)
```
